32 devices in a mesh: data: 4 (over z), cp: 8 (over y, x, core).
Axes of the slice: x: 2, y: 2, z: 4, core: 2. Of those that a mesh axis runs over, the one named last changes fastest.
Arguments:
- q: bfloat16 [4, 2048, 32, 128], P('data', 'cp'), parts along dimension 0
- k: bfloat16 [4, 2048, 32, 128], P('data', 'cp'), parts along dimension 0
- v: bfloat16 [4, 2048, 32, 128], P('data', 'cp'), parts along dimension 0
- o: bfloat16 [4, 2048, 32, 128], P('data', 'cp'), parts along dimension 0
- lse: float32 [4, 32, 2048], P('data', None, 'cp'), parts along dimension 0
- do: bfloat16 [4, 2048, 32, 128], P('data', 'cp'), parts along dimension 0
Outputs:
- output 1: bfloat16 [4, 2048, 32, 128], P('data', 'cp'), parts along dimension 0
- output 2: bfloat16 [4, 2048, 32, 128], P('data', 'cp'), parts along dimension 0
- output 3: bfloat16 [4, 2048, 32, 128], P('data', 'cp'), parts along dimension 0
There are 4 independent parts. The reference program is written for one: setup_inputs(seed, part) draws one part's arguments, and reference() takes and returns one part's arrays. A program takes and returns all parts, laid end to end along the dimension named above; each array names one.
All inputs are finite; a program needn't handle non-finite values.
Results may differ from the reference program's by a relative error of at most 0.001.
Values are sent between devices in bfloat16 or wider.
A program may use at most 1 GiB of HBM per device.

```python
import jax
import jax.numpy as jnp
from jax import lax
import numpy as np

CP = 8
BATCH = 1
TOKENS_DEV = 256
HEADS = 32
HEAD = 128


def _positions():
    c = TOKENS_DEV // 2
    dev = np.arange(CP)[:, None]
    u = np.arange(c)[None, :]
    return np.concatenate([dev * c + u, (2 * CP - 1 - dev) * c + u], axis=1).reshape(2 * CP, c)


def _segments(x):
    c = TOKENS_DEV // 2
    return jnp.moveaxis(x.astype(jnp.float32).reshape(BATCH, 2 * CP, c, HEADS, HEAD), 1, 0)


def _forward(q, k, v):
    c = TOKENS_DEV // 2
    scale = HEAD ** -0.5
    pos = jnp.asarray(_positions(), dtype=jnp.int32)
    qs, ks, vs = _segments(q), _segments(k), _segments(v)

    def one(xs):
        qb, pq = xs

        def scores(kb, pk):
            s = jnp.einsum('bqhd,bkhd->bhqk', qb, kb) * scale
            return jnp.where(pq[:, None] >= pk[None, :], s, -jnp.inf)

        def stat(carry, ys):
            m, l = carry
            s = scores(*ys)
            m2 = jnp.maximum(m, jnp.max(s, axis=-1))
            return (m2, l * jnp.exp(m - m2) + jnp.sum(jnp.exp(s - m2[..., None]), axis=-1)), None

        m0 = jnp.full((BATCH, HEADS, c), -jnp.inf, jnp.float32)
        (m, l), _ = lax.scan(stat, (m0, jnp.zeros_like(m0)), (ks, pos))
        lse = m + jnp.log(l)

        def acc(o, ys):
            kb, vb, pk = ys
            p = jnp.exp(scores(kb, pk) - lse[..., None])
            return o + jnp.einsum('bhqk,bkhd->bqhd', p, vb), None

        o, _ = lax.scan(acc, jnp.zeros((BATCH, c, HEADS, HEAD), jnp.float32), (ks, vs, pos))
        return o, lse

    o, lse = lax.map(one, (qs, pos))
    o = jnp.moveaxis(o, 0, 1).reshape(BATCH, CP * TOKENS_DEV, HEADS, HEAD).astype(jnp.bfloat16)
    lse = jnp.moveaxis(lse, 0, 2).reshape(BATCH, HEADS, CP * TOKENS_DEV)
    return o, lse


def setup_inputs(seed: int = 0, part: int = 0) -> dict:
    key = jax.random.fold_in(jax.random.PRNGKey(seed), part)
    kq, kk, kv, kd = jax.random.split(key, 4)
    shape = (BATCH, CP * TOKENS_DEV, HEADS, HEAD)
    q = jax.random.normal(kq, shape, jnp.float32).astype(jnp.bfloat16)
    k = jax.random.normal(kk, shape, jnp.float32).astype(jnp.bfloat16)
    v = jax.random.normal(kv, shape, jnp.float32).astype(jnp.bfloat16)
    do = jax.random.normal(kd, shape, jnp.float32).astype(jnp.bfloat16)
    o, lse = _forward(q, k, v)
    return {'q': q, 'k': k, 'v': v, 'o': o, 'lse': lse, 'do': do}


def reference(q, k, v, o, lse, do):
    nseg = 2 * CP
    c = TOKENS_DEV // 2
    scale = HEAD ** -0.5
    pos = jnp.asarray(_positions(), dtype=jnp.int32)
    qs, ks, vs, dos = _segments(q), _segments(k), _segments(v), _segments(do)
    delta = jnp.sum(do.astype(jnp.float32) * o.astype(jnp.float32), axis=-1)
    deltas = jnp.moveaxis(jnp.swapaxes(delta, 1, 2).reshape(BATCH, HEADS, nseg, c), 2, 0)
    lses = jnp.moveaxis(lse.reshape(BATCH, HEADS, nseg, c), 2, 0)

    def per_query(carry, xs):
        dk, dv = carry
        qb, dob, lb, db, pq = xs

        def per_key(ys):
            kb, vb, pk = ys
            s = jnp.einsum('bqhd,bkhd->bhqk', qb, kb) * scale
            p = jnp.where(pq[:, None] >= pk[None, :], jnp.exp(s - lb[..., None]), 0.0)
            dvb = jnp.einsum('bhqk,bqhd->bkhd', p.astype(jnp.bfloat16).astype(jnp.float32), dob)
            dp = jnp.einsum('bqhd,bkhd->bhqk', dob, vb)
            ds = (p * (dp - db[..., None])).astype(jnp.bfloat16).astype(jnp.float32)
            return jnp.einsum('bhqk,bkhd->bqhd', ds, kb), jnp.einsum('bhqk,bqhd->bkhd', ds, qb), dvb

        dqs, dks, dvs = lax.map(per_key, (ks, vs, pos))
        return (dk + dks, dv + dvs), jnp.sum(dqs, axis=0)

    zero = jnp.zeros_like(ks)
    (dk, dv), dq = lax.scan(per_query, (zero, zero), (qs, dos, lses, deltas, pos))

    def unseg(x):
        return jnp.moveaxis(x, 0, 1).reshape(BATCH, CP * TOKENS_DEV, HEADS, HEAD).astype(jnp.bfloat16)

    return unseg(dq * scale), unseg(dk * scale), unseg(dv)
```

```python
import functools

import jax
import jax.numpy as jnp
from jax import lax
from jax.experimental import pallas as pl
from jax.experimental.pallas import tpu as pltpu
from jax.sharding import PartitionSpec as P

F32 = jnp.float32
BF16 = jnp.bfloat16
MESH = pl.DeviceIdType.MESH
LOG2E = 1.4426950408889634

N = 8
SEG = 128
NSEG = 16
BLK = 512
FLIPS = ((0, 1, 0), (1, 0, 0), (1, 1, 0), (0, 1, 1), (1, 0, 1), (1, 1, 1), (0, 0, 1))


def _flip(d, flips):
    fy, fx, fc = flips
    if fy:
        d = (d + 4) % 8
    if fx:
        d = d + 2 - 4 * ((d // 2) % 2)
    if fc:
        d = d + 1 - 2 * (d % 2)
    return d


def _nt(a, b):
    return lax.dot_general(a, b, (((1,), (1,)), ((), ())), preferred_element_type=F32)


def _tn(a, b):
    return lax.dot_general(a, b, (((0,), (0,)), ((), ())), preferred_element_type=F32)


def _nn(a, b):
    return lax.dot_general(a, b, (((1,), (0,)), ((), ())), preferred_element_type=F32)


def _kernel(hl, scale, q, k, v, do, ld, dq, dk, dv, xin, ldin, obuf, dqacc, dkacc, dvacc,
            send_in, recv_in, send_ld, recv_ld, send_out, recv_out):
    me = lax.axis_index('cp')
    peers = [_flip(me, f) for f in FLIPS]

    barrier = pltpu.get_barrier_semaphore()
    for p in peers:
        pl.semaphore_signal(barrier, inc=1, device_id={'cp': p}, device_id_type=MESH)
    pl.semaphore_wait(barrier, N - 1)

    lo = pl.ds(pl.multiple_of(me * SEG, SEG), SEG)
    hi = pl.ds(pl.multiple_of((NSEG - 1 - me) * SEG, SEG), SEG)

    for half, seg in ((0, me), (1, NSEG - 1 - me)):
        for n, p in enumerate(peers):
            pltpu.make_async_remote_copy(ld.at[p, half], ldin.at[seg], send_ld, recv_ld,
                                         device_id={'cp': p}, device_id_type=MESH).start()
        pltpu.make_async_copy(ld.at[me, half], ldin.at[seg], recv_ld).start()

    for h in range(hl):
        for t, x in enumerate((q, k, v, do)):
            for half, rows in ((0, lo), (1, hi)):
                src = x.at[me * hl + h, pl.ds(half * SEG, SEG)]
                pltpu.make_async_copy(src, xin.at[h, t, rows], recv_in.at[h]).start()
        for p in peers:
            for t, x in enumerate((q, k, v, do)):
                for half, rows in ((0, lo), (1, hi)):
                    src = x.at[p * hl + h, pl.ds(half * SEG, SEG)]
                    pltpu.make_async_remote_copy(src, xin.at[h, t, rows], send_in, recv_in.at[h],
                                                 device_id={'cp': p}, device_id_type=MESH).start()

    pltpu.make_async_copy(ldin, ldin, recv_ld).wait()

    nblk = NSEG * SEG // BLK
    per = BLK // SEG

    def head(h, carry):
        pltpu.make_async_copy(xin.at[h], xin.at[h], recv_in.at[h]).wait()
        dqacc[...] = jnp.zeros_like(dqacc)

        for j in range(nblk):
            kr = pl.ds(j * BLK, BLK)

            def tile(i, masked):
                qr = pl.ds(pl.multiple_of(i * BLK, BLK), BLK)
                qb, dob = xin[h, 0, qr, :], xin[h, 3, qr, :]
                kb, vb = xin[h, 1, kr, :], xin[h, 2, kr, :]
                l2 = jnp.concatenate([ldin[i * per + s, pl.ds(2 * h, 1), :] for s in range(per)], axis=1)
                dl = jnp.concatenate([ldin[i * per + s, pl.ds(2 * h + 1, 1), :] for s in range(per)], axis=1)
                p = jnp.exp2(_nt(kb, qb) * (scale * LOG2E) - l2)
                if masked:
                    key = lax.broadcasted_iota(jnp.int32, (BLK, BLK), 0)
                    query = lax.broadcasted_iota(jnp.int32, (BLK, BLK), 1)
                    p = jnp.where(key <= query, p, 0.0)
                ds = (p * (_nt(vb, dob) - dl)).astype(BF16)
                dvb = _nn(p.astype(BF16), dob)
                dkb = _nn(ds, qb)
                dqacc[qr, :] += _tn(ds, kb)
                return dkb, dvb

            dkb, dvb = tile(j, True)
            dkacc[...] = dkb
            dvacc[...] = dvb

            @pl.loop(j + 1, nblk)
            def _(i):
                dkb, dvb = tile(i, False)
                dkacc[...] += dkb
                dvacc[...] += dvb

            obuf[h, 1, kr, :] = (dkacc[...] * scale).astype(BF16)
            obuf[h, 2, kr, :] = dvacc[...].astype(BF16)
        obuf[h, 0] = (dqacc[...] * scale).astype(BF16)

        mine = me * hl + h
        for p in peers:
            for t, x in enumerate((dq, dk, dv)):
                for half, seg in ((0, p), (1, NSEG - 1 - p)):
                    src = obuf.at[h, t, pl.ds(pl.multiple_of(seg * SEG, SEG), SEG)]
                    pltpu.make_async_remote_copy(src, x.at[mine, pl.ds(half * SEG, SEG)], send_out, recv_out.at[t],
                                                 device_id={'cp': p}, device_id_type=MESH).start()
        for t, x in enumerate((dq, dk, dv)):
            for half, rows in ((0, lo), (1, hi)):
                pltpu.make_async_copy(obuf.at[h, t, rows], x.at[mine, pl.ds(half * SEG, SEG)], recv_out.at[t]).start()
        return carry

    lax.fori_loop(0, hl, head, 0)

    far = pl.ds(0, (N - 1) * NSEG * SEG // N)
    pltpu.make_async_copy(ldin.at[pl.ds(0, 2 * (N - 1))], ldin.at[pl.ds(0, 2 * (N - 1))], send_ld).wait()
    pltpu.make_async_copy(xin.at[:, :, far], xin.at[:, :, far], send_in).wait()
    pltpu.make_async_copy(obuf.at[:, :, far], obuf.at[:, :, far], send_out).wait()
    for t, x in enumerate((dq, dk, dv)):
        pltpu.make_async_copy(x, x, recv_out.at[t]).wait()


def solution(mesh):
    spec = P('data', 'cp', None, None)
    lspec = P('data', None, 'cp')

    def local(q, k, v, o, lse, do):
        b, tok, heads, dim = q.shape
        hl = heads // N
        delta = jnp.einsum('bqhd,bqhd->bhq', do, o, preferred_element_type=F32)[0]
        ld = jnp.stack([lse[0] * LOG2E, delta], axis=1).reshape(N, 2 * hl, 2, SEG).transpose(0, 2, 1, 3)
        qt, kt, vt, dot = (jnp.swapaxes(x[0], 0, 1) for x in (q, k, v, do))
        any_ = pl.BlockSpec(memory_space=pl.ANY)
        seq = NSEG * SEG
        outs = pl.pallas_call(
            functools.partial(_kernel, hl, dim ** -0.5),
            out_shape=[jax.ShapeDtypeStruct((heads, tok, dim), BF16)] * 3,
            in_specs=[any_] * 5,
            out_specs=[any_] * 3,
            scratch_shapes=[
                pltpu.VMEM((hl, 4, seq, dim), BF16),
                pltpu.VMEM((NSEG, 2 * hl, SEG), F32),
                pltpu.VMEM((hl, 3, seq, dim), BF16),
                pltpu.VMEM((seq, dim), F32),
                pltpu.VMEM((BLK, dim), F32),
                pltpu.VMEM((BLK, dim), F32),
                pltpu.SemaphoreType.DMA,
                pltpu.SemaphoreType.DMA((hl,)),
                pltpu.SemaphoreType.DMA,
                pltpu.SemaphoreType.DMA,
                pltpu.SemaphoreType.DMA,
                pltpu.SemaphoreType.DMA((3,)),
            ],
            compiler_params=pltpu.CompilerParams(collective_id=0, has_side_effects=True,
                                                 vmem_limit_bytes=56 * 2 ** 20),
            name='attention_backward',
        )(qt, kt, vt, dot, ld)
        return tuple(jnp.swapaxes(x, 0, 1)[None] for x in outs)

    return jax.shard_map(local, mesh=mesh, in_specs=(spec, spec, spec, spec, lspec, spec),
                         out_specs=(spec, spec, spec), check_vma=False)
```

```python
import functools

import jax
import jax.numpy as jnp
from jax import lax
from jax.experimental import pallas as pl
from jax.experimental.pallas import tpu as pltpu
from jax.sharding import PartitionSpec as P

F32 = jnp.float32
BF16 = jnp.bfloat16
MESH = pl.DeviceIdType.MESH
LOG2E = 1.4426950408889634

N = 8
SEG = 128
NSEG = 16
BLK = 512
CHIPS = ((0, 1), (1, 0), (1, 1), (0, 0))
CHUNK = 64


def _chip(c, flips):
    fy, fx = flips
    if fy:
        c = (c + 2) % 4
    if fx:
        c = c + 1 - 2 * (c % 2)
    return c


def _nt(a, b):
    return lax.dot_general(a, b, (((1,), (1,)), ((), ())), preferred_element_type=F32)


def _tn(a, b):
    return lax.dot_general(a, b, (((0,), (0,)), ((), ())), preferred_element_type=F32)


def _nn(a, b):
    return lax.dot_general(a, b, (((1,), (0,)), ((), ())), preferred_element_type=F32)


def _swap(dst, src, tok, inverse=False):
    @pl.loop(0, tok // CHUNK)
    def _(i):
        r = pl.ds(pl.multiple_of(i * CHUNK, CHUNK), CHUNK)
        if inverse:
            dst[r] = jnp.swapaxes(src[:, r, :], 0, 1)
        else:
            dst[:, r, :] = jnp.swapaxes(src[r], 0, 1)


def _kernel(hl, scale, q, k, v, do, o, lse, dq, dk, dv, nat, onat, lsev, hm, ohm, ldst, xin, ldin, obuf, rin,
            dqacc, dkacc, dvacc, nat_sem, lse_sem, send_in, recv_in, send_ld, recv_ld, send_out, recv_out):
    me = lax.axis_index('cp')
    core = me % 2
    chips = [_chip(me // 2, f) for f in CHIPS]
    tok = nat.shape[2]
    peers = [[2 * chip + b for b in (0, 1)] for chip in chips]
    other = me + 1 - 2 * core
    remote = [p for ps in peers[:3] for p in ps] + [other]

    barrier = pltpu.get_barrier_semaphore()
    for p in remote:
        pl.semaphore_signal(barrier, inc=1, device_id={'cp': p}, device_id_type=MESH)

    inputs = (q, k, v, do)
    group = [pl.ds(pl.multiple_of(chip * 2 * hl, 2 * hl), 2 * hl) for chip in chips]

    def load(t, c):
        return pltpu.make_async_copy(inputs[t].at[:, group[c]], nat.at[t, c], nat_sem.at[t, c])

    def load_o(c):
        return pltpu.make_async_copy(o.at[:, group[c]], onat.at[c], nat_sem.at[4, c])

    for t in range(4):
        for c in range(4):
            load(t, c).start()
    for c in range(4):
        load_o(c).start()
    load_lse = pltpu.make_async_copy(lse, lsev, lse_sem)
    load_lse.start()

    segs = (me, NSEG - 1 - me)
    rows = [pl.ds(pl.multiple_of(s * SEG, SEG), SEG) for s in segs]
    halves = [pl.ds(half * SEG, SEG) for half in (0, 1)]

    def send(t, c, h):
        for half in (0, 1):
            dst = xin.at[h, t, rows[half]]
            if c < 3:
                for b in (0, 1):
                    pltpu.make_async_remote_copy(hm.at[t, c, b * hl + h, halves[half]], dst, send_in, recv_in.at[h],
                                                 device_id={'cp': peers[c][b]}, device_id_type=MESH).start()
            else:
                pltpu.make_async_remote_copy(hm.at[t, c, (1 - core) * hl + h, halves[half]], dst, send_in, recv_in.at[h],
                                             device_id={'cp': other}, device_id_type=MESH).start()
                pltpu.make_async_copy(hm.at[t, c, core * hl + h, halves[half]], dst, recv_in.at[h]).start()

    units = [(t, c) for t in range(4) for c in range(4)]
    for n, (t, c) in enumerate(units):
        load(t, c).wait()
        _swap(hm.at[t, c], nat.at[t, c], tok)
        if n == 0:
            pl.semaphore_wait(barrier, N - 1)
        else:
            send(*units[n - 1], 0)

    row = lax.broadcasted_iota(jnp.int32, (2 * hl, nat.shape[-1]), 0)
    load_lse.wait()
    for c in range(4):
        load_o(c).wait()
        _swap(ohm, onat.at[c], tok)
        if c == 0:
            send(*units[-1], 0)
        delta = jnp.zeros((2 * hl, tok), F32)
        for g in range(2 * hl):
            prod = hm[3, c, g].astype(F32) * ohm[g].astype(F32)
            top = prod.astype(BF16)
            low = (prod - top.astype(F32)).astype(BF16)
            pick = jnp.where(row == g, 1.0, 0.0).astype(BF16)
            delta = delta + (_nt(pick, top) + _nt(pick, low))
        l2 = lsev[group[c], :] * LOG2E
        for b in (0, 1):
            for half in (0, 1):
                ldst[c, b, half, 0:hl, :] = l2[b * hl:(b + 1) * hl, half * SEG:(half + 1) * SEG]
                ldst[c, b, half, hl:2 * hl, :] = delta[b * hl:(b + 1) * hl, half * SEG:(half + 1) * SEG]
    for half in (0, 1):
        dst = ldin.at[segs[half]]
        for c in range(3):
            for b in (0, 1):
                pltpu.make_async_remote_copy(ldst.at[c, b, half], dst, send_ld, recv_ld,
                                             device_id={'cp': peers[c][b]}, device_id_type=MESH).start()
        pltpu.make_async_remote_copy(ldst.at[3, 1 - core, half], dst, send_ld, recv_ld,
                                     device_id={'cp': other}, device_id_type=MESH).start()
        pltpu.make_async_copy(ldst.at[3, core, half], dst, recv_ld).start()
    for h in range(1, hl):
        for c in range(4):
            for t in range(4):
                send(t, c, h)

    pltpu.make_async_copy(ldin, ldin, recv_ld).wait()

    nblk = NSEG * SEG // BLK
    per = BLK // SEG

    def head(h, carry):
        pltpu.make_async_copy(xin.at[h], xin.at[h], recv_in.at[h]).wait()
        dqacc[...] = jnp.zeros_like(dqacc)

        for j in range(nblk):
            kr = pl.ds(j * BLK, BLK)

            def tile(i, masked):
                qr = pl.ds(pl.multiple_of(i * BLK, BLK), BLK)
                qb, dob = xin[h, 0, qr, :], xin[h, 3, qr, :]
                kb, vb = xin[h, 1, kr, :], xin[h, 2, kr, :]
                l2 = jnp.concatenate([ldin[i * per + s, pl.ds(h, 1), :] for s in range(per)], axis=1)
                dl = jnp.concatenate([ldin[i * per + s, pl.ds(hl + h, 1), :] for s in range(per)], axis=1)
                p = jnp.exp2(_nt(kb, qb) * (scale * LOG2E) - l2)
                if masked:
                    key = lax.broadcasted_iota(jnp.int32, (BLK, BLK), 0)
                    query = lax.broadcasted_iota(jnp.int32, (BLK, BLK), 1)
                    p = jnp.where(key <= query, p, 0.0)
                ds = (p * (_nt(vb, dob) - dl)).astype(BF16)
                dvb = _nn(p.astype(BF16), dob)
                dkb = _nn(ds, qb)
                dqacc[qr, :] += _tn(ds, kb)
                return dkb, dvb

            dkb, dvb = tile(j, True)
            dkacc[...] = dkb
            dvacc[...] = dvb

            @pl.loop(j + 1, nblk)
            def _(i):
                dkb, dvb = tile(i, False)
                dkacc[...] += dkb
                dvacc[...] += dvb

            obuf[h, 1, kr, :] = (dkacc[...] * scale).astype(BF16)
            obuf[h, 2, kr, :] = dvacc[...].astype(BF16)
        obuf[h, 0] = (dqacc[...] * scale).astype(BF16)

        mine = me * hl + h
        for t in (1, 2, 0):
            for p in remote:
                for half, seg in ((0, p), (1, NSEG - 1 - p)):
                    src = obuf.at[h, t, pl.ds(pl.multiple_of(seg * SEG, SEG), SEG)]
                    pltpu.make_async_remote_copy(src, rin.at[t, mine, halves[half]], send_out, recv_out.at[t],
                                                 device_id={'cp': p}, device_id_type=MESH).start()
            for half in (0, 1):
                pltpu.make_async_copy(obuf.at[h, t, rows[half]], rin.at[t, mine, halves[half]], recv_out.at[t]).start()
        return carry

    lax.fori_loop(0, hl, head, 0)

    for t, x in ((1, dk), (2, dv), (0, dq)):
        pltpu.make_async_copy(rin.at[t], rin.at[t], recv_out.at[t]).wait()
        for g in range(N // 2):
            heads = pl.ds(g * 2 * hl, 2 * hl)
            _swap(x.at[:, heads], rin.at[t, heads], tok, inverse=True)
    far = pl.ds(0, (N - 1) * NSEG * SEG // N)
    pltpu.make_async_copy(ldin.at[pl.ds(0, 2 * (N - 1))], ldin.at[pl.ds(0, 2 * (N - 1))], send_ld).wait()
    pltpu.make_async_copy(xin.at[:, :, far], xin.at[:, :, far], send_in).wait()
    pltpu.make_async_copy(obuf.at[:, :, far], obuf.at[:, :, far], send_out).wait()


def solution(mesh):
    spec = P('data', 'cp', None, None)
    lspec = P('data', None, 'cp')

    def local(q, k, v, o, lse, do):
        b, tok, heads, dim = q.shape
        hl = heads // N
        any_ = pl.BlockSpec(memory_space=pltpu.HBM)
        seq = NSEG * SEG
        outs = pl.pallas_call(
            functools.partial(_kernel, hl, dim ** -0.5),
            out_shape=[jax.ShapeDtypeStruct((tok, heads, dim), BF16)] * 3,
            in_specs=[any_] * 6,
            out_specs=[pl.BlockSpec(memory_space=pltpu.VMEM)] * 3,
            scratch_shapes=[
                pltpu.VMEM((4, N // 2, tok, 2 * hl, dim), BF16),
                pltpu.VMEM((N // 2, tok, 2 * hl, dim), BF16),
                pltpu.VMEM((heads, tok), F32),
                pltpu.VMEM((4, N // 2, 2 * hl, tok, dim), BF16),
                pltpu.VMEM((2 * hl, tok, dim), BF16),
                pltpu.VMEM((N // 2, 2, 2, 2 * hl, SEG), F32),
                pltpu.VMEM((hl, 4, seq, dim), BF16),
                pltpu.VMEM((NSEG, 2 * hl, SEG), F32),
                pltpu.VMEM((hl, 3, seq, dim), BF16),
                pltpu.VMEM((3, heads, tok, dim), BF16),
                pltpu.VMEM((seq, dim), F32),
                pltpu.VMEM((BLK, dim), F32),
                pltpu.VMEM((BLK, dim), F32),
                pltpu.SemaphoreType.DMA((5, N // 2)),
                pltpu.SemaphoreType.DMA,
                pltpu.SemaphoreType.DMA,
                pltpu.SemaphoreType.DMA((hl,)),
                pltpu.SemaphoreType.DMA,
                pltpu.SemaphoreType.DMA,
                pltpu.SemaphoreType.DMA,
                pltpu.SemaphoreType.DMA((3,)),
            ],
            compiler_params=pltpu.CompilerParams(collective_id=0, has_side_effects=True,
                                                 vmem_limit_bytes=47 * 2 ** 20),
            name='attention_backward',
        )(q[0], k[0], v[0], do[0], o[0], lse[0])
        return tuple(x[None] for x in outs)

    return jax.shard_map(local, mesh=mesh, in_specs=(spec, spec, spec, spec, lspec, spec),
                         out_specs=(spec, spec, spec), check_vma=False)
```

```python
import functools

import jax
import jax.numpy as jnp
from jax import lax
from jax.experimental import pallas as pl
from jax.experimental.pallas import tpu as pltpu
from jax.sharding import PartitionSpec as P

F32 = jnp.float32
BF16 = jnp.bfloat16
MESH = pl.DeviceIdType.MESH
LOG2E = 1.4426950408889634

N = 8
SEG = 128
NSEG = 16
BLK = 512
CHIPS = ((0, 1), (1, 0), (1, 1), (0, 0))
CHUNK = 64
AHEAD = 4


def _chip(c, flips):
    fy, fx = flips
    if fy:
        c = (c + 2) % 4
    if fx:
        c = c + 1 - 2 * (c % 2)
    return c


def _nt(a, b):
    return lax.dot_general(a, b, (((1,), (1,)), ((), ())), preferred_element_type=F32)


def _tn(a, b):
    return lax.dot_general(a, b, (((0,), (0,)), ((), ())), preferred_element_type=F32)


def _nn(a, b):
    return lax.dot_general(a, b, (((1,), (0,)), ((), ())), preferred_element_type=F32)


def _swap(dst, src, tok, inverse=False):
    @pl.loop(0, tok // CHUNK)
    def _(i):
        r = pl.ds(pl.multiple_of(i * CHUNK, CHUNK), CHUNK)
        if inverse:
            dst[r] = jnp.swapaxes(src[:, r, :], 0, 1)
        else:
            dst[:, r, :] = jnp.swapaxes(src[r], 0, 1)


def _kernel(hl, scale, q, k, v, do, o, lse, dqh, dk, dv, nat, onat, lsev, hm, ohm, ldst, xin, ldin, obuf, rin,
            dqacc, dkacc, dvacc, nat_sem, lse_sem, send_in, recv_in, send_ld, recv_ld, send_out, recv_out):
    me = lax.axis_index('cp')
    core = me % 2
    chips = [_chip(me // 2, f) for f in CHIPS]
    tok = nat.shape[2]
    peers = [[2 * chip + b for b in (0, 1)] for chip in chips]
    other = me + 1 - 2 * core
    remote = [p for ps in peers[:3] for p in ps] + [other]

    barrier = pltpu.get_barrier_semaphore()
    for p in remote:
        pl.semaphore_signal(barrier, inc=1, device_id={'cp': p}, device_id_type=MESH)

    inputs = (q, k, v, do)
    group = [pl.ds(pl.multiple_of(chip * 2 * hl, 2 * hl), 2 * hl) for chip in chips]

    def load(t, c):
        return pltpu.make_async_copy(inputs[t].at[:, group[c]], nat.at[t, c], nat_sem.at[t, c])

    def load_o(c):
        return pltpu.make_async_copy(o.at[:, group[c]], onat.at[c], nat_sem.at[4, c])

    units = [(t, c) for t in range(4) for c in range(4)]
    loads = [load(*u) for u in units] + [load_o(c) for c in range(4)]
    for copy in loads[:AHEAD]:
        copy.start()
    load_lse = pltpu.make_async_copy(lse, lsev, lse_sem)
    load_lse.start()

    segs = (me, NSEG - 1 - me)
    rows = [pl.ds(pl.multiple_of(s * SEG, SEG), SEG) for s in segs]
    halves = [pl.ds(half * SEG, SEG) for half in (0, 1)]

    def send(t, c, h):
        for half in (0, 1):
            dst = xin.at[h, t, rows[half]]
            if c < 3:
                for b in (0, 1):
                    pltpu.make_async_remote_copy(hm.at[t, c, b * hl + h, halves[half]], dst, send_in, recv_in.at[h],
                                                 device_id={'cp': peers[c][b]}, device_id_type=MESH).start()
            else:
                pltpu.make_async_remote_copy(hm.at[t, c, (1 - core) * hl + h, halves[half]], dst, send_in, recv_in.at[h],
                                             device_id={'cp': other}, device_id_type=MESH).start()
                pltpu.make_async_copy(hm.at[t, c, core * hl + h, halves[half]], dst, recv_in.at[h]).start()

    for n, (t, c) in enumerate(units):
        if n + AHEAD < len(loads):
            loads[n + AHEAD].start()
        loads[n].wait()
        _swap(hm.at[t, c], nat.at[t, c], tok)
        if n == 0:
            pl.semaphore_wait(barrier, N - 1)
        else:
            send(*units[n - 1], 0)

    row = lax.broadcasted_iota(jnp.int32, (2 * hl, nat.shape[-1]), 0)
    load_lse.wait()
    for c in range(4):
        loads[16 + c].wait()
        _swap(ohm, onat.at[c], tok)
        if c == 0:
            send(*units[-1], 0)
        delta = jnp.zeros((2 * hl, tok), F32)
        for g in range(2 * hl):
            prod = hm[3, c, g].astype(F32) * ohm[g].astype(F32)
            top = prod.astype(BF16)
            low = (prod - top.astype(F32)).astype(BF16)
            pick = jnp.where(row == g, 1.0, 0.0).astype(BF16)
            delta = delta + (_nt(pick, top) + _nt(pick, low))
        l2 = lsev[group[c], :] * LOG2E
        for b in (0, 1):
            for half in (0, 1):
                ldst[c, b, half, 0:hl, :] = l2[b * hl:(b + 1) * hl, half * SEG:(half + 1) * SEG]
                ldst[c, b, half, hl:2 * hl, :] = delta[b * hl:(b + 1) * hl, half * SEG:(half + 1) * SEG]
    for half in (0, 1):
        dst = ldin.at[segs[half]]
        for c in range(3):
            for b in (0, 1):
                pltpu.make_async_remote_copy(ldst.at[c, b, half], dst, send_ld, recv_ld,
                                             device_id={'cp': peers[c][b]}, device_id_type=MESH).start()
        pltpu.make_async_remote_copy(ldst.at[3, 1 - core, half], dst, send_ld, recv_ld,
                                     device_id={'cp': other}, device_id_type=MESH).start()
        pltpu.make_async_copy(ldst.at[3, core, half], dst, recv_ld).start()
    for h in range(1, hl):
        for c in range(4):
            for t in range(4):
                send(t, c, h)

    pltpu.make_async_copy(ldin, ldin, recv_ld).wait()

    nblk = NSEG * SEG // BLK
    per = BLK // SEG

    def head(h, carry):
        pltpu.make_async_copy(xin.at[h], xin.at[h], recv_in.at[h]).wait()
        dqacc[...] = jnp.zeros_like(dqacc)

        for j in range(nblk):
            kr = pl.ds(j * BLK, BLK)

            def tile(i, masked):
                qr = pl.ds(pl.multiple_of(i * BLK, BLK), BLK)
                qb, dob = xin[h, 0, qr, :], xin[h, 3, qr, :]
                kb, vb = xin[h, 1, kr, :], xin[h, 2, kr, :]
                l2 = jnp.concatenate([ldin[i * per + s, pl.ds(h, 1), :] for s in range(per)], axis=1)
                dl = jnp.concatenate([ldin[i * per + s, pl.ds(hl + h, 1), :] for s in range(per)], axis=1)
                p = jnp.exp2(_nt(kb, qb) * (scale * LOG2E) - l2)
                if masked:
                    key = lax.broadcasted_iota(jnp.int32, (BLK, BLK), 0)
                    query = lax.broadcasted_iota(jnp.int32, (BLK, BLK), 1)
                    p = jnp.where(key <= query, p, 0.0)
                ds = (p * (_nt(vb, dob) - dl)).astype(BF16)
                dvb = _nn(p.astype(BF16), dob)
                dkb = _nn(ds, qb)
                dqacc[qr, :] += _tn(ds, kb)
                return dkb, dvb

            dkb, dvb = tile(j, True)
            dkacc[...] = dkb
            dvacc[...] = dvb

            @pl.loop(j + 1, nblk)
            def _(i):
                dkb, dvb = tile(i, False)
                dkacc[...] += dkb
                dvacc[...] += dvb

            obuf[h, 1, kr, :] = (dkacc[...] * scale).astype(BF16)
            obuf[h, 2, kr, :] = dvacc[...].astype(BF16)
        obuf[h, 0] = (dqacc[...] * scale).astype(BF16)

        mine = me * hl + h
        for t, x in ((1, rin.at[0]), (2, rin.at[1]), (0, dqh)):
            for p in remote:
                for half, seg in ((0, p), (1, NSEG - 1 - p)):
                    src = obuf.at[h, t, pl.ds(pl.multiple_of(seg * SEG, SEG), SEG)]
                    pltpu.make_async_remote_copy(src, x.at[mine, halves[half]], send_out, recv_out.at[t],
                                                 device_id={'cp': p}, device_id_type=MESH).start()
            for half in (0, 1):
                pltpu.make_async_copy(obuf.at[h, t, rows[half]], x.at[mine, halves[half]], recv_out.at[t]).start()
        return carry

    lax.fori_loop(0, hl, head, 0)

    for t, x in ((1, dk), (2, dv)):
        src = rin.at[t - 1]
        pltpu.make_async_copy(src, src, recv_out.at[t]).wait()
        for g in range(N // 2):
            heads = pl.ds(g * 2 * hl, 2 * hl)
            _swap(x.at[:, heads], src.at[heads], tok, inverse=True)
    pltpu.make_async_copy(dqh, dqh, recv_out.at[0]).wait()
    far = pl.ds(0, (N - 1) * NSEG * SEG // N)
    pltpu.make_async_copy(ldin.at[pl.ds(0, 2 * (N - 1))], ldin.at[pl.ds(0, 2 * (N - 1))], send_ld).wait()
    pltpu.make_async_copy(xin.at[:, :, far], xin.at[:, :, far], send_in).wait()
    pltpu.make_async_copy(obuf.at[:, :, far], obuf.at[:, :, far], send_out).wait()


def _close(dqh, dkt, dvt, dq, dk, dv, dqt, sem):
    copies = [pltpu.make_async_copy(dkt, dk, sem.at[0]), pltpu.make_async_copy(dvt, dv, sem.at[1])]
    for copy in copies:
        copy.start()
    heads, tok = dqh.shape[:2]
    for g in range(heads // 8):
        part = pl.ds(g * 8, 8)
        _swap(dqt.at[g], dqh.at[part], tok, inverse=True)
        copies.append(pltpu.make_async_copy(dqt.at[g], dq.at[:, part], sem.at[2 + g]))
        copies[-1].start()
    for copy in copies:
        copy.wait()


def solution(mesh):
    spec = P('data', 'cp', None, None)
    lspec = P('data', None, 'cp')

    def local(q, k, v, o, lse, do):
        b, tok, heads, dim = q.shape
        hl = heads // N
        any_ = pl.BlockSpec(memory_space=pltpu.HBM)
        vmem = pl.BlockSpec(memory_space=pltpu.VMEM)
        seq = NSEG * SEG
        outs = pl.pallas_call(
            functools.partial(_kernel, hl, dim ** -0.5),
            out_shape=[jax.ShapeDtypeStruct((heads, tok, dim), BF16)] + [jax.ShapeDtypeStruct((tok, heads, dim), BF16)] * 2,
            in_specs=[any_] * 6,
            out_specs=[vmem] * 3,
            scratch_shapes=[
                pltpu.VMEM((4, N // 2, tok, 2 * hl, dim), BF16),
                pltpu.VMEM((N // 2, tok, 2 * hl, dim), BF16),
                pltpu.VMEM((heads, tok), F32),
                pltpu.VMEM((4, N // 2, 2 * hl, tok, dim), BF16),
                pltpu.VMEM((2 * hl, tok, dim), BF16),
                pltpu.VMEM((N // 2, 2, 2, 2 * hl, SEG), F32),
                pltpu.VMEM((hl, 4, seq, dim), BF16),
                pltpu.VMEM((NSEG, 2 * hl, SEG), F32),
                pltpu.VMEM((hl, 3, seq, dim), BF16),
                pltpu.VMEM((2, heads, tok, dim), BF16),
                pltpu.VMEM((seq, dim), F32),
                pltpu.VMEM((BLK, dim), F32),
                pltpu.VMEM((BLK, dim), F32),
                pltpu.SemaphoreType.DMA((5, N // 2)),
                pltpu.SemaphoreType.DMA,
                pltpu.SemaphoreType.DMA,
                pltpu.SemaphoreType.DMA((hl,)),
                pltpu.SemaphoreType.DMA,
                pltpu.SemaphoreType.DMA,
                pltpu.SemaphoreType.DMA,
                pltpu.SemaphoreType.DMA((3,)),
            ],
            compiler_params=pltpu.CompilerParams(collective_id=0, has_side_effects=True,
                                                 vmem_limit_bytes=46 * 2 ** 20),
            name='attention_backward',
        )(q[0], k[0], v[0], do[0], o[0], lse[0])
        grads = pl.pallas_call(
            _close,
            out_shape=[jax.ShapeDtypeStruct((tok, heads, dim), BF16)] * 3,
            in_specs=[vmem] * 3,
            out_specs=[any_] * 3,
            scratch_shapes=[pltpu.VMEM((heads // 8, tok, 8, dim), BF16),
                            pltpu.SemaphoreType.DMA((2 + heads // 8,))],
            compiler_params=pltpu.CompilerParams(vmem_limit_bytes=16 * 2 ** 20),
            name='close',
        )(*outs)
        return tuple(x[None] for x in grads)

    return jax.shard_map(local, mesh=mesh, in_specs=(spec, spec, spec, spec, lspec, spec),
                         out_specs=(spec, spec, spec), check_vma=False)
```

```python
import functools

import jax
import jax.numpy as jnp
from jax import lax
from jax.experimental import pallas as pl
from jax.experimental.pallas import tpu as pltpu
from jax.sharding import PartitionSpec as P

F32 = jnp.float32
BF16 = jnp.bfloat16
MESH = pl.DeviceIdType.MESH
LOG2E = 1.4426950408889634

N = 8
SEG = 128
NSEG = 16
BLK = 512
CHIPS = ((0, 1), (1, 0), (1, 1), (0, 0))
CHUNK = 64
AHEAD = 4
RING = 6


def _chip(c, flips):
    fy, fx = flips
    if fy:
        c = (c + 2) % 4
    if fx:
        c = c + 1 - 2 * (c % 2)
    return c


def _nt(a, b):
    return lax.dot_general(a, b, (((1,), (1,)), ((), ())), preferred_element_type=F32)


def _tn(a, b):
    return lax.dot_general(a, b, (((0,), (0,)), ((), ())), preferred_element_type=F32)


def _nn(a, b):
    return lax.dot_general(a, b, (((1,), (0,)), ((), ())), preferred_element_type=F32)


def _swap(dst, src, tok, inverse=False):
    @pl.loop(0, tok // CHUNK)
    def _(i):
        r = pl.ds(pl.multiple_of(i * CHUNK, CHUNK), CHUNK)
        if inverse:
            dst[r] = jnp.swapaxes(src[:, r, :], 0, 1)
        else:
            dst[:, r, :] = jnp.swapaxes(src[r], 0, 1)


def _kernel(hl, scale, q, k, v, do, o, lse, dqh, dk, dv, nat, lsev, hm, ohm, ldst, xin, ldin, obuf, rin,
            dqacc, dkacc, dvacc, rel, loc, locld, lkv, ldq, gdq, rdq, fdq,
            nat_sem, lse_sem, send_in, recv_in, send_ld, recv_ld, send_out, recv_out,
            rel_sem, fwd_sem, send_loc, recv_loc, gdq_sem, send_fdq, rdq_sem):
    me = lax.axis_index('cp')
    core = me % 2
    chip = me // 2
    chips = [_chip(chip, f) for f in CHIPS]
    tok = nat.shape[1]
    outer = chip != 0
    last = pl.ds((NSEG - 2) * SEG, 2 * SEG)
    peers = [[2 * chip + b for b in (0, 1)] for chip in chips]
    other = me + 1 - 2 * core
    remote = [p for ps in peers[:3] for p in ps] + [other]

    barrier = pltpu.get_barrier_semaphore()
    for p in remote:
        pl.semaphore_signal(barrier, inc=1, device_id={'cp': p}, device_id_type=MESH)

    inputs = (q, k, v, do)
    group = [pl.ds(pl.multiple_of(chip * 2 * hl, 2 * hl), 2 * hl) for chip in chips]

    units = [(t, c) for t in range(4) for c in range(4)]
    loads = [pltpu.make_async_copy(x.at[:, group[c]], nat.at[(4 * t + c) % RING], nat_sem.at[(4 * t + c) % RING])
             for t, x in enumerate((*inputs, o)) for c in range(4)]
    for copy in loads[:AHEAD]:
        copy.start()
    load_lse = pltpu.make_async_copy(lse, lsev, lse_sem)
    load_lse.start()

    segs = (me, NSEG - 1 - me)
    rows = [pl.ds(pl.multiple_of(s * SEG, SEG), SEG) for s in segs]
    halves = [pl.ds(half * SEG, SEG) for half in (0, 1)]

    def send(t, c, h):
        for half in (0, 1):
            dst = xin.at[h, t, rows[half]]
            if c < 3:
                go = me >= 0
                if t in (1, 2) and half == 1:
                    go = outer
                if (t, c, h) in relayed:
                    go = jnp.logical_and(go, chip != 2)

                @pl.when(go)
                def _():
                    for b in (0, 1):
                        pltpu.make_async_remote_copy(hm.at[t, c, b * hl + h, halves[half]], dst, send_in, recv_in.at[h],
                                                     device_id={'cp': peers[c][b]}, device_id_type=MESH).start()
            else:
                pltpu.make_async_remote_copy(hm.at[t, c, (1 - core) * hl + h, halves[half]], dst, send_in, recv_in.at[h],
                                             device_id={'cp': other}, device_id_type=MESH).start()
                pltpu.make_async_copy(hm.at[t, c, core * hl + h, halves[half]], dst, recv_in.at[h]).start()

    relayed = [(t, 2, hl - 1) for t in (0, 1)]

    def forward():
        pltpu.make_async_copy(rel, rel, rel_sem).wait()
        for t in (0, 1):
            for b in (0, 1):
                for half, seg in ((0, me + 4), (1, NSEG - 5 - me)):
                    dst = xin.at[hl - 1, t, pl.ds(pl.multiple_of(seg * SEG, SEG), SEG)]
                    pltpu.make_async_remote_copy(rel.at[t, b, halves[half]], dst, fwd_sem, recv_in.at[hl - 1],
                                                 device_id={'cp': 2 + b}, device_id_type=MESH).start()

    @pl.when(outer)
    def _():
        for h in range(hl):
            for t in (1, 2):
                xin[h, t, last, :] = jnp.zeros((2 * SEG, xin.shape[-1]), BF16)

    for n, (t, c) in enumerate(units):
        if n + AHEAD < len(loads):
            loads[n + AHEAD].start()
        loads[n].wait()
        _swap(hm.at[t, c], nat.at[n % RING], tok)
        if n == 0:
            pl.semaphore_wait(barrier, N - 1)
        else:
            send(*units[n - 1], 0)

    row = lax.broadcasted_iota(jnp.int32, (2 * hl, nat.shape[-1]), 0)
    load_lse.wait()
    for c in range(4):
        loads[16 + c].wait()
        _swap(ohm, nat.at[(16 + c) % RING], tok)
        if c == 0:
            send(*units[-1], 0)
        delta = jnp.zeros((2 * hl, tok), F32)
        for g in range(2 * hl):
            prod = hm[3, c, g].astype(F32) * ohm[g].astype(F32)
            top = prod.astype(BF16)
            low = (prod - top.astype(F32)).astype(BF16)
            pick = jnp.where(row == g, 1.0, 0.0).astype(BF16)
            delta = delta + (_nt(pick, top) + _nt(pick, low))
        l2 = lsev[group[c], :] * LOG2E
        for b in (0, 1):
            for half in (0, 1):
                ldst[c, b, half, 0:hl, :] = l2[b * hl:(b + 1) * hl, half * SEG:(half + 1) * SEG]
                ldst[c, b, half, hl:2 * hl, :] = delta[b * hl:(b + 1) * hl, half * SEG:(half + 1) * SEG]
    for half in (0, 1):
        dst = ldin.at[segs[half]]
        for c in range(3):
            for b in (0, 1):
                pltpu.make_async_remote_copy(ldst.at[c, b, half], dst, send_ld, recv_ld,
                                             device_id={'cp': peers[c][b]}, device_id_type=MESH).start()
        pltpu.make_async_remote_copy(ldst.at[3, 1 - core, half], dst, send_ld, recv_ld,
                                     device_id={'cp': other}, device_id_type=MESH).start()
        pltpu.make_async_copy(ldst.at[3, core, half], dst, recv_ld).start()

    @pl.when(chip == 2)
    def _():
        for t in (0, 1):
            for b in (0, 1):
                pltpu.make_async_remote_copy(hm.at[t, 2, b * hl + hl - 1], rel.at[t, b], send_in, rel_sem,
                                             device_id={'cp': 2 * chips[1] + core}, device_id_type=MESH).start()

    own_rows = pl.ds(pl.multiple_of((1 - core) * SEG, SEG), SEG)
    other_rows = pl.ds(pl.multiple_of(core * SEG, SEG), SEG)
    own_heads = pl.ds(core * hl, hl)
    other_heads = pl.ds((1 - core) * hl, hl)

    @pl.when(chip == 0)
    def _():
        for c in range(3):
            for t in range(4):
                dst = loc.at[c, t, :, own_rows]
                pltpu.make_async_copy(hm.at[t, c, own_heads, halves[1]], dst, recv_loc.at[0]).start()
                pltpu.make_async_remote_copy(hm.at[t, c, other_heads, halves[1]], dst, send_loc.at[0], recv_loc.at[0],
                                             device_id={'cp': other}, device_id_type=MESH).start()
            dst = locld.at[c, 1 - core]
            pltpu.make_async_copy(ldst.at[c, core, 1], dst, recv_loc.at[1]).start()
            pltpu.make_async_remote_copy(ldst.at[c, 1 - core, 1], dst, send_loc.at[1], recv_loc.at[1],
                                         device_id={'cp': other}, device_id_type=MESH).start()

    for h in range(1, hl):
        for c in range(4):
            for t in range(4):
                send(t, c, h)

    @pl.when(chip == 0)
    def _():
        pltpu.make_async_copy(loc, loc, recv_loc.at[0]).wait()
        pltpu.make_async_copy(locld, locld, recv_loc.at[1]).wait()

        @pl.loop(0, 3 * hl)
        def _(i):
            c, h = i // hl, i % hl
            qb, kb, vb, dob = (loc[c, t, h] for t in range(4))
            l2 = jnp.concatenate([locld[c, s, pl.ds(h, 1), :] for s in (0, 1)], axis=1)
            dl = jnp.concatenate([locld[c, s, pl.ds(hl + h, 1), :] for s in (0, 1)], axis=1)
            p = jnp.exp2(_nt(kb, qb) * (scale * LOG2E) - l2)
            key = lax.broadcasted_iota(jnp.int32, p.shape, 0)
            query = lax.broadcasted_iota(jnp.int32, p.shape, 1)
            p = jnp.where(key <= query, p, 0.0)
            ds = (p * (_nt(vb, dob) - dl)).astype(BF16)
            lkv[0, c, h] = (_nn(ds, qb) * scale).astype(BF16)
            lkv[1, c, h] = _nn(p.astype(BF16), dob).astype(BF16)
            ldq[c, h] = _tn(ds, kb)

        for c in range(3):
            heads = pl.ds((2 * chips[c] + core) * hl, hl)
            for t in (0, 1):
                dst = rin.at[t, heads, halves[1]]
                pltpu.make_async_copy(lkv.at[t, c, :, own_rows], dst, recv_out.at[t + 1]).start()
                pltpu.make_async_remote_copy(lkv.at[t, c, :, other_rows], dst, send_loc.at[2], recv_out.at[t + 1],
                                             device_id={'cp': other}, device_id_type=MESH).start()
            dst = gdq.at[c, core]
            pltpu.make_async_copy(ldq.at[c, :, own_rows], dst, gdq_sem).start()
            pltpu.make_async_remote_copy(ldq.at[c, :, other_rows], dst, send_loc.at[3], gdq_sem,
                                         device_id={'cp': other}, device_id_type=MESH).start()

    pltpu.make_async_copy(ldin, ldin, recv_ld).wait()

    nblk = NSEG * SEG // BLK
    per = BLK // SEG
    keys = jnp.where(outer, BLK - 2 * SEG, BLK)

    def head(h, carry):
        @pl.when(outer)
        def _():
            most = xin.at[h, :, pl.ds(0, (NSEG - 1) * SEG)]
            pltpu.make_async_copy(most, most, recv_in.at[h]).wait()

        @pl.when(chip == 0)
        def _():
            pltpu.make_async_copy(xin.at[h], xin.at[h], recv_in.at[h]).wait()

        dqacc[...] = jnp.zeros_like(dqacc)

        for j in range(nblk):
            kr = pl.ds(j * BLK, BLK)

            def tile(i, masked):
                qr = pl.ds(pl.multiple_of(i * BLK, BLK), BLK)
                qb, dob = xin[h, 0, qr, :], xin[h, 3, qr, :]
                kb, vb = xin[h, 1, kr, :], xin[h, 2, kr, :]
                l2 = jnp.concatenate([ldin[i * per + s, pl.ds(h, 1), :] for s in range(per)], axis=1)
                dl = jnp.concatenate([ldin[i * per + s, pl.ds(hl + h, 1), :] for s in range(per)], axis=1)
                p = jnp.exp2(_nt(kb, qb) * (scale * LOG2E) - l2)
                if masked:
                    key = lax.broadcasted_iota(jnp.int32, (BLK, BLK), 0)
                    query = lax.broadcasted_iota(jnp.int32, (BLK, BLK), 1)
                    seen = key <= query
                    if j == nblk - 1:
                        seen = jnp.logical_and(seen, key < keys)
                    p = jnp.where(seen, p, 0.0)
                ds = (p * (_nt(vb, dob) - dl)).astype(BF16)
                dvb = _nn(p.astype(BF16), dob)
                dkb = _nn(ds, qb)
                dqacc[qr, :] += _tn(ds, kb)
                return dkb, dvb

            dkb, dvb = tile(j, True)
            dkacc[...] = dkb
            dvacc[...] = dvb

            @pl.loop(j + 1, nblk)
            def _(i):
                dkb, dvb = tile(i, False)
                dkacc[...] += dkb
                dvacc[...] += dvb

            obuf[h, 1, kr, :] = (dkacc[...] * scale).astype(BF16)
            obuf[h, 2, kr, :] = dvacc[...].astype(BF16)
        obuf[h, 0] = (dqacc[...] * scale).astype(BF16)

        @pl.when(outer)
        def _():
            fdq[h] = dqacc[last, :]
            for b in (0, 1):
                pltpu.make_async_remote_copy(fdq.at[h, pl.ds((1 - b) * SEG, SEG)], rdq.at[chip - 1, core, h], send_fdq, rdq_sem,
                                             device_id={'cp': b}, device_id_type=MESH).start()

        @pl.when(jnp.logical_and(chip == 0, h == 0))
        def _():
            forward()

        mine = me * hl + h
        for t, x in ((1, rin.at[0]), (2, rin.at[1]), (0, dqh)):
            for p in remote:
                for half, seg in ((0, p), (1, NSEG - 1 - p)):
                    src = obuf.at[h, t, pl.ds(pl.multiple_of(seg * SEG, SEG), SEG)]
                    go = me >= 0
                    if half == 1:
                        go = jnp.logical_not(jnp.logical_and(outer, p < 2))

                    @pl.when(go)
                    def _():
                        pltpu.make_async_remote_copy(src, x.at[mine, halves[half]], send_out, recv_out.at[t],
                                                     device_id={'cp': p}, device_id_type=MESH).start()
            for half in (0, 1):
                pltpu.make_async_copy(obuf.at[h, t, rows[half]], x.at[mine, halves[half]], recv_out.at[t]).start()
        return carry

    lax.fori_loop(0, hl, head, 0)

    for t, x in ((1, dk), (2, dv)):
        src = rin.at[t - 1]
        pltpu.make_async_copy(src, src, recv_out.at[t]).wait()
        for g in range(N // 2):
            heads = pl.ds(g * 2 * hl, 2 * hl)
            _swap(x.at[:, heads], src.at[heads], tok, inverse=True)

    @pl.when(chip == 0)
    def _():
        pltpu.make_async_copy(gdq, gdq, gdq_sem).wait()
        pltpu.make_async_copy(rdq, rdq, rdq_sem).wait()

        @pl.loop(0, 6 * hl)
        def _(i):
            c, r = i // (2 * hl), i % (2 * hl)
            total = gdq[c, r // hl, r % hl] + rdq[c, r // hl, r % hl]
            dqh[2 * hl + i, halves[1], :] = (total * scale).astype(BF16)

        some = dqh.at[pl.ds(0, 5 * hl)]
        pltpu.make_async_copy(some, some, recv_out.at[0]).wait()
        for n, ref in enumerate((loc.at[:, :, :, halves[0]], locld.at[:, 0], lkv.at[:, :, :, halves[0]], ldq.at[:, :, halves[0]])):
            pltpu.make_async_copy(ref, ref, send_loc.at[n]).wait()
        pltpu.make_async_copy(rel, rel, fwd_sem).wait()
        sent = xin.at[:, :, pl.ds(0, 11 * SEG)]
        pltpu.make_async_copy(sent, sent, send_in).wait()
        sent = obuf.at[:, :, pl.ds(0, 14 * SEG)]
        pltpu.make_async_copy(sent, sent, send_out).wait()

    @pl.when(outer)
    def _():
        pltpu.make_async_copy(dqh, dqh, recv_out.at[0]).wait()
        pltpu.make_async_copy(fdq, fdq, send_fdq).wait()
        sent = xin.at[:, :, pl.ds(0, 14 * SEG)]
        pltpu.make_async_copy(sent, sent, send_in).wait()
        sent = obuf.at[:, :, pl.ds(0, 12 * SEG)]
        pltpu.make_async_copy(sent, sent, send_out).wait()

    pltpu.make_async_copy(ldin.at[pl.ds(0, 2 * (N - 1))], ldin.at[pl.ds(0, 2 * (N - 1))], send_ld).wait()


def _close(dqh, dkt, dvt, dq, dk, dv, dqt, sem):
    copies = [pltpu.make_async_copy(dkt, dk, sem.at[0]), pltpu.make_async_copy(dvt, dv, sem.at[1])]
    for copy in copies:
        copy.start()
    heads, tok = dqh.shape[:2]
    for g in range(heads // 8):
        part = pl.ds(g * 8, 8)
        _swap(dqt.at[g], dqh.at[part], tok, inverse=True)
        copies.append(pltpu.make_async_copy(dqt.at[g], dq.at[:, part], sem.at[2 + g]))
        copies[-1].start()
    for copy in copies:
        copy.wait()


def solution(mesh):
    spec = P('data', 'cp', None, None)
    lspec = P('data', None, 'cp')

    def local(q, k, v, o, lse, do):
        b, tok, heads, dim = q.shape
        hl = heads // N
        any_ = pl.BlockSpec(memory_space=pltpu.HBM)
        vmem = pl.BlockSpec(memory_space=pltpu.VMEM)
        seq = NSEG * SEG
        outs = pl.pallas_call(
            functools.partial(_kernel, hl, dim ** -0.5),
            out_shape=[jax.ShapeDtypeStruct((heads, tok, dim), BF16)] + [jax.ShapeDtypeStruct((tok, heads, dim), BF16)] * 2,
            in_specs=[any_] * 6,
            out_specs=[vmem] * 3,
            scratch_shapes=[
                pltpu.VMEM((RING, tok, 2 * hl, dim), BF16),
                pltpu.VMEM((heads, tok), F32),
                pltpu.VMEM((4, N // 2, 2 * hl, tok, dim), BF16),
                pltpu.VMEM((2 * hl, tok, dim), BF16),
                pltpu.VMEM((N // 2, 2, 2, 2 * hl, SEG), F32),
                pltpu.VMEM((hl, 4, seq, dim), BF16),
                pltpu.VMEM((NSEG, 2 * hl, SEG), F32),
                pltpu.VMEM((hl, 3, seq, dim), BF16),
                pltpu.VMEM((2, heads, tok, dim), BF16),
                pltpu.VMEM((seq, dim), F32),
                pltpu.VMEM((BLK, dim), F32),
                pltpu.VMEM((BLK, dim), F32),
                pltpu.VMEM((2, 2, tok, dim), BF16),
                pltpu.VMEM((3, 4, hl, 2 * SEG, dim), BF16),
                pltpu.VMEM((3, 2, 2 * hl, SEG), F32),
                pltpu.VMEM((2, 3, hl, 2 * SEG, dim), BF16),
                pltpu.VMEM((3, hl, 2 * SEG, dim), F32),
                pltpu.VMEM((3, 2, hl, SEG, dim), F32),
                pltpu.VMEM((3, 2, hl, SEG, dim), F32),
                pltpu.VMEM((hl, 2 * SEG, dim), F32),
                pltpu.SemaphoreType.DMA((RING,)),
                pltpu.SemaphoreType.DMA,
                pltpu.SemaphoreType.DMA,
                pltpu.SemaphoreType.DMA((hl,)),
                pltpu.SemaphoreType.DMA,
                pltpu.SemaphoreType.DMA,
                pltpu.SemaphoreType.DMA,
                pltpu.SemaphoreType.DMA((3,)),
                pltpu.SemaphoreType.DMA,
                pltpu.SemaphoreType.DMA,
                pltpu.SemaphoreType.DMA((4,)),
                pltpu.SemaphoreType.DMA((2,)),
                pltpu.SemaphoreType.DMA,
                pltpu.SemaphoreType.DMA,
                pltpu.SemaphoreType.DMA,
            ],
            compiler_params=pltpu.CompilerParams(collective_id=0, has_side_effects=True,
                                                 vmem_limit_bytes=46 * 2 ** 20),
            name='attention_backward',
        )(q[0], k[0], v[0], do[0], o[0], lse[0])
        grads = pl.pallas_call(
            _close,
            out_shape=[jax.ShapeDtypeStruct((tok, heads, dim), BF16)] * 3,
            in_specs=[vmem] * 3,
            out_specs=[any_] * 3,
            scratch_shapes=[pltpu.VMEM((heads // 8, tok, 8, dim), BF16),
                            pltpu.SemaphoreType.DMA((2 + heads // 8,))],
            compiler_params=pltpu.CompilerParams(vmem_limit_bytes=16 * 2 ** 20),
            name='close',
        )(*outs)
        return tuple(x[None] for x in grads)

    return jax.shard_map(local, mesh=mesh, in_specs=(spec, spec, spec, spec, lspec, spec),
                         out_specs=(spec, spec, spec), check_vma=False)
```

```python
import functools

import jax
import jax.numpy as jnp
from jax import lax
from jax.experimental import pallas as pl
from jax.experimental.pallas import tpu as pltpu
from jax.sharding import PartitionSpec as P

F32 = jnp.float32
BF16 = jnp.bfloat16
MESH = pl.DeviceIdType.MESH
LOG2E = 1.4426950408889634

N = 8
SEG = 128
NSEG = 16
BLK = 512
CHIPS = ((0, 1), (1, 0), (1, 1), (0, 0))
CHUNK = 64
AHEAD = 4
RING = 6


def _chip(c, flips):
    fy, fx = flips
    if fy:
        c = (c + 2) % 4
    if fx:
        c = c + 1 - 2 * (c % 2)
    return c


def _nt(a, b):
    return lax.dot_general(a, b, (((1,), (1,)), ((), ())), preferred_element_type=F32)


def _tn(a, b):
    return lax.dot_general(a, b, (((0,), (0,)), ((), ())), preferred_element_type=F32)


def _nn(a, b):
    return lax.dot_general(a, b, (((1,), (0,)), ((), ())), preferred_element_type=F32)


def _swap(dst, src, tok, inverse=False):
    @pl.loop(0, tok // CHUNK)
    def _(i):
        r = pl.ds(pl.multiple_of(i * CHUNK, CHUNK), CHUNK)
        if inverse:
            dst[r] = jnp.swapaxes(src[:, r, :], 0, 1)
        else:
            dst[:, r, :] = jnp.swapaxes(src[r], 0, 1)


def _kernel(hl, scale, q, k, v, do, o, lse, dqh, dk, dv, nat, lsev, hm, ohm, ldst, xin, ldin, obuf, rin,
            dqacc, dkacc, dvacc, rel, loc, locld, lkv, ldq, gdq, rdq, fdq, pdq,
            nat_sem, lse_sem, send_in, recv_in, send_ld, recv_ld, send_out, recv_out,
            rel_sem, fwd_sem, send_loc, recv_loc, gdq_sem, send_fdq, rdq_sem, pdq_sem, send_pdq):
    me = lax.axis_index('cp')
    core = me % 2
    chip = me // 2
    chips = [_chip(chip, f) for f in CHIPS]
    tok = nat.shape[1]
    outer = chip != 0
    first = pl.ds(0, hl - 1)
    last = pl.ds((NSEG - 2) * SEG, 2 * SEG)
    peers = [[2 * chip + b for b in (0, 1)] for chip in chips]
    other = me + 1 - 2 * core
    remote = [p for ps in peers[:3] for p in ps] + [other]

    barrier = pltpu.get_barrier_semaphore()
    for p in remote:
        pl.semaphore_signal(barrier, inc=1, device_id={'cp': p}, device_id_type=MESH)

    inputs = (q, k, v, do)
    group = [pl.ds(pl.multiple_of(chip * 2 * hl, 2 * hl), 2 * hl) for chip in chips]

    units = [(t, c) for t in range(4) for c in range(4)]
    loads = [pltpu.make_async_copy(x.at[:, group[c]], nat.at[(4 * t + c) % RING], nat_sem.at[(4 * t + c) % RING])
             for t, x in enumerate((*inputs, o)) for c in range(4)]
    for copy in loads[:AHEAD]:
        copy.start()
    load_lse = pltpu.make_async_copy(lse, lsev, lse_sem)
    load_lse.start()

    segs = (me, NSEG - 1 - me)
    rows = [pl.ds(pl.multiple_of(s * SEG, SEG), SEG) for s in segs]
    halves = [pl.ds(half * SEG, SEG) for half in (0, 1)]

    def send(t, c, h):
        for half in (0, 1):
            dst = xin.at[h, t, rows[half]]
            if c < 3:
                for b in (0, 1):
                    go = outer if t in (1, 2) and half == 1 else me >= 0
                    if c == 2 and h == hl - 1 and (t, b) in relayed:
                        go = jnp.logical_and(go, chip != 2)

                    @pl.when(go)
                    def _():
                        pltpu.make_async_remote_copy(hm.at[t, c, b * hl + h, halves[half]], dst, send_in, recv_in.at[h],
                                                     device_id={'cp': peers[c][b]}, device_id_type=MESH).start()
            else:
                pltpu.make_async_remote_copy(hm.at[t, c, (1 - core) * hl + h, halves[half]], dst, send_in, recv_in.at[h],
                                             device_id={'cp': other}, device_id_type=MESH).start()
                pltpu.make_async_copy(hm.at[t, c, core * hl + h, halves[half]], dst, recv_in.at[h]).start()

    relayed = [(0, 0), (0, 1), (1, 0), (1, 1), (2, 0)]

    def forward():
        pltpu.make_async_copy(rel, rel, rel_sem).wait()
        for n, (t, b) in enumerate(relayed):
            for half, seg in ((0, me + 4), (1, NSEG - 5 - me)):
                dst = xin.at[hl - 1, t, pl.ds(pl.multiple_of(seg * SEG, SEG), SEG)]
                pltpu.make_async_remote_copy(rel.at[n, halves[half]], dst, fwd_sem, recv_in.at[hl - 1],
                                             device_id={'cp': 2 + b}, device_id_type=MESH).start()

    @pl.when(outer)
    def _():
        for h in range(hl):
            for t in (1, 2):
                xin[h, t, last, :] = jnp.zeros((2 * SEG, xin.shape[-1]), BF16)

    for n, (t, c) in enumerate(units):
        if n + AHEAD < len(loads):
            loads[n + AHEAD].start()
        loads[n].wait()
        _swap(hm.at[t, c], nat.at[n % RING], tok)
        if n == 0:
            pl.semaphore_wait(barrier, N - 1)
        else:
            send(*units[n - 1], 0)

    row = lax.broadcasted_iota(jnp.int32, (2 * hl, nat.shape[-1]), 0)
    load_lse.wait()
    for c in range(4):
        loads[16 + c].wait()
        _swap(ohm, nat.at[(16 + c) % RING], tok)
        if c == 0:
            send(*units[-1], 0)
        delta = jnp.zeros((2 * hl, tok), F32)
        for g in range(2 * hl):
            prod = hm[3, c, g].astype(F32) * ohm[g].astype(F32)
            top = prod.astype(BF16)
            low = (prod - top.astype(F32)).astype(BF16)
            pick = jnp.where(row == g, 1.0, 0.0).astype(BF16)
            delta = delta + (_nt(pick, top) + _nt(pick, low))
        l2 = lsev[group[c], :] * LOG2E
        for b in (0, 1):
            for half in (0, 1):
                ldst[c, b, half, 0:hl, :] = l2[b * hl:(b + 1) * hl, half * SEG:(half + 1) * SEG]
                ldst[c, b, half, hl:2 * hl, :] = delta[b * hl:(b + 1) * hl, half * SEG:(half + 1) * SEG]
    for half in (0, 1):
        dst = ldin.at[segs[half]]
        for c in range(3):
            for b in (0, 1):
                pltpu.make_async_remote_copy(ldst.at[c, b, half], dst, send_ld, recv_ld,
                                             device_id={'cp': peers[c][b]}, device_id_type=MESH).start()
        pltpu.make_async_remote_copy(ldst.at[3, 1 - core, half], dst, send_ld, recv_ld,
                                     device_id={'cp': other}, device_id_type=MESH).start()
        pltpu.make_async_copy(ldst.at[3, core, half], dst, recv_ld).start()

    @pl.when(chip == 2)
    def _():
        for n, (t, b) in enumerate(relayed):
            pltpu.make_async_remote_copy(hm.at[t, 2, b * hl + hl - 1], rel.at[n], send_in, rel_sem,
                                         device_id={'cp': 2 * chips[1] + core}, device_id_type=MESH).start()

    own_rows = pl.ds(pl.multiple_of((1 - core) * SEG, SEG), SEG)
    other_rows = pl.ds(pl.multiple_of(core * SEG, SEG), SEG)
    own_heads = pl.ds(core * hl, hl)
    other_heads = pl.ds((1 - core) * hl, hl)

    @pl.when(chip == 0)
    def _():
        for c in range(3):
            for t in range(4):
                dst = loc.at[c, t, :, own_rows]
                pltpu.make_async_copy(hm.at[t, c, own_heads, halves[1]], dst, recv_loc.at[0]).start()
                pltpu.make_async_remote_copy(hm.at[t, c, other_heads, halves[1]], dst, send_loc.at[0], recv_loc.at[0],
                                             device_id={'cp': other}, device_id_type=MESH).start()
            dst = locld.at[c, 1 - core]
            pltpu.make_async_copy(ldst.at[c, core, 1], dst, recv_loc.at[1]).start()
            pltpu.make_async_remote_copy(ldst.at[c, 1 - core, 1], dst, send_loc.at[1], recv_loc.at[1],
                                         device_id={'cp': other}, device_id_type=MESH).start()

    for h in range(1, hl):
        for c in range(4):
            for t in range(4):
                send(t, c, h)

    @pl.when(chip == 0)
    def _():
        pltpu.make_async_copy(loc, loc, recv_loc.at[0]).wait()
        pltpu.make_async_copy(locld, locld, recv_loc.at[1]).wait()

        @pl.loop(0, 3 * hl)
        def _(i):
            c, h = i // hl, i % hl
            qb, kb, vb, dob = (loc[c, t, h] for t in range(4))
            l2 = jnp.concatenate([locld[c, s, pl.ds(h, 1), :] for s in (0, 1)], axis=1)
            dl = jnp.concatenate([locld[c, s, pl.ds(hl + h, 1), :] for s in (0, 1)], axis=1)
            p = jnp.exp2(_nt(kb, qb) * (scale * LOG2E) - l2)
            key = lax.broadcasted_iota(jnp.int32, p.shape, 0)
            query = lax.broadcasted_iota(jnp.int32, p.shape, 1)
            p = jnp.where(key <= query, p, 0.0)
            ds = (p * (_nt(vb, dob) - dl)).astype(BF16)
            lkv[0, c, h] = (_nn(ds, qb) * scale).astype(BF16)
            lkv[1, c, h] = _nn(p.astype(BF16), dob).astype(BF16)
            ldq[c, h] = _tn(ds, kb)

        for c in range(3):
            heads = pl.ds((2 * chips[c] + core) * hl, hl)
            for t in (0, 1):
                dst = rin.at[t, heads, halves[1]]
                pltpu.make_async_copy(lkv.at[t, c, :, own_rows], dst, recv_out.at[t + 1]).start()
                pltpu.make_async_remote_copy(lkv.at[t, c, :, other_rows], dst, send_loc.at[2], recv_out.at[t + 1],
                                             device_id={'cp': other}, device_id_type=MESH).start()
            dst = gdq.at[c, core]
            pltpu.make_async_copy(ldq.at[c, first, own_rows], dst, gdq_sem).start()
            pltpu.make_async_remote_copy(ldq.at[c, first, other_rows], dst, send_loc.at[3], gdq_sem,
                                         device_id={'cp': other}, device_id_type=MESH).start()
            pltpu.make_async_remote_copy(ldq.at[c, hl - 1], pdq, send_pdq, pdq_sem,
                                         device_id={'cp': peers[c][0] + core}, device_id_type=MESH).start()

    pltpu.make_async_copy(ldin, ldin, recv_ld).wait()

    nblk = NSEG * SEG // BLK
    per = BLK // SEG
    keys = jnp.where(outer, BLK - 2 * SEG, BLK)

    def head(h, carry):
        @pl.when(outer)
        def _():
            most = xin.at[h, :, pl.ds(0, (NSEG - 1) * SEG)]
            pltpu.make_async_copy(most, most, recv_in.at[h]).wait()

        @pl.when(chip == 0)
        def _():
            pltpu.make_async_copy(xin.at[h], xin.at[h], recv_in.at[h]).wait()

        dqacc[...] = jnp.zeros_like(dqacc)

        for j in range(nblk):
            kr = pl.ds(j * BLK, BLK)

            def tile(i, masked):
                qr = pl.ds(pl.multiple_of(i * BLK, BLK), BLK)
                qb, dob = xin[h, 0, qr, :], xin[h, 3, qr, :]
                kb, vb = xin[h, 1, kr, :], xin[h, 2, kr, :]
                l2 = jnp.concatenate([ldin[i * per + s, pl.ds(h, 1), :] for s in range(per)], axis=1)
                dl = jnp.concatenate([ldin[i * per + s, pl.ds(hl + h, 1), :] for s in range(per)], axis=1)
                p = jnp.exp2(_nt(kb, qb) * (scale * LOG2E) - l2)
                if masked:
                    key = lax.broadcasted_iota(jnp.int32, (BLK, BLK), 0)
                    query = lax.broadcasted_iota(jnp.int32, (BLK, BLK), 1)
                    seen = key <= query
                    if j == nblk - 1:
                        seen = jnp.logical_and(seen, key < keys)
                    p = jnp.where(seen, p, 0.0)
                ds = (p * (_nt(vb, dob) - dl)).astype(BF16)
                dvb = _nn(p.astype(BF16), dob)
                dkb = _nn(ds, qb)
                dqacc[qr, :] += _tn(ds, kb)
                return dkb, dvb

            dkb, dvb = tile(j, True)
            dkacc[...] = dkb
            dvacc[...] = dvb

            @pl.loop(j + 1, nblk)
            def _(i):
                dkb, dvb = tile(i, False)
                dkacc[...] += dkb
                dvacc[...] += dvb

            obuf[h, 1, kr, :] = (dkacc[...] * scale).astype(BF16)
            obuf[h, 2, kr, :] = dvacc[...].astype(BF16)

        @pl.when(jnp.logical_and(outer, h == hl - 1))
        def _():
            pltpu.make_async_copy(pdq, pdq, pdq_sem).wait()
            dqacc[last, :] += pdq[...]

        obuf[h, 0] = (dqacc[...] * scale).astype(BF16)

        @pl.when(jnp.logical_and(outer, h < hl - 1))
        def _():
            fdq[h] = dqacc[last, :]
            for b in (0, 1):
                pltpu.make_async_remote_copy(fdq.at[h, pl.ds((1 - b) * SEG, SEG)], rdq.at[chip - 1, core, h], send_fdq, rdq_sem,
                                             device_id={'cp': b}, device_id_type=MESH).start()

        @pl.when(jnp.logical_and(chip == 0, h == 0))
        def _():
            forward()

        mine = me * hl + h
        for t, x in ((1, rin.at[0]), (2, rin.at[1]), (0, dqh)):
            for p in remote:
                for half, seg in ((0, p), (1, NSEG - 1 - p)):
                    src = obuf.at[h, t, pl.ds(pl.multiple_of(seg * SEG, SEG), SEG)]
                    go = me >= 0
                    if half == 1:
                        go = jnp.logical_not(jnp.logical_and(outer, p < 2))

                    @pl.when(go)
                    def _():
                        pltpu.make_async_remote_copy(src, x.at[mine, halves[half]], send_out, recv_out.at[t],
                                                     device_id={'cp': p}, device_id_type=MESH).start()

                    if half == 1 and t == 0:
                        @pl.when(jnp.logical_and(jnp.logical_not(go), h == hl - 1))
                        def _():
                            pltpu.make_async_remote_copy(src, x.at[mine, halves[half]], send_pdq, recv_out.at[t],
                                                         device_id={'cp': p}, device_id_type=MESH).start()
            for half in (0, 1):
                pltpu.make_async_copy(obuf.at[h, t, rows[half]], x.at[mine, halves[half]], recv_out.at[t]).start()
        return carry

    lax.fori_loop(0, hl, head, 0)

    for t, x in ((1, dk), (2, dv)):
        src = rin.at[t - 1]
        pltpu.make_async_copy(src, src, recv_out.at[t]).wait()
        for g in range(N // 2):
            heads = pl.ds(g * 2 * hl, 2 * hl)
            _swap(x.at[:, heads], src.at[heads], tok, inverse=True)

    @pl.when(chip == 0)
    def _():
        pltpu.make_async_copy(gdq, gdq, gdq_sem).wait()
        pltpu.make_async_copy(rdq, rdq, rdq_sem).wait()

        few = hl - 1

        @pl.loop(0, 6 * few)
        def _(i):
            c, b, h = i // (2 * few), (i // few) % 2, i % few
            total = gdq[c, b, h] + rdq[c, b, h]
            dqh[(2 * c + 2 + b) * hl + h, halves[1], :] = (total * scale).astype(BF16)

        some = dqh.at[pl.ds(0, 2 * N * hl // 2 - 3 * few)]
        pltpu.make_async_copy(some, some, recv_out.at[0]).wait()
        pltpu.make_async_copy(ldq.at[:, hl - 1], ldq.at[:, hl - 1], send_pdq).wait()
        for n, ref in enumerate((loc.at[:, :, :, halves[0]], locld.at[:, 0], lkv.at[:, :, :, halves[0]], ldq.at[:, first, halves[0]])):
            pltpu.make_async_copy(ref, ref, send_loc.at[n]).wait()
        pltpu.make_async_copy(rel, rel, fwd_sem).wait()
        sent = xin.at[:, :, pl.ds(0, 11 * SEG)]
        pltpu.make_async_copy(sent, sent, send_in).wait()
        sent = obuf.at[:, :, pl.ds(0, 14 * SEG)]
        pltpu.make_async_copy(sent, sent, send_out).wait()

    @pl.when(outer)
    def _():
        pltpu.make_async_copy(dqh, dqh, recv_out.at[0]).wait()
        pltpu.make_async_copy(fdq, fdq, send_fdq).wait()
        sent = obuf.at[hl - 1, 0, last]
        pltpu.make_async_copy(sent, sent, send_pdq).wait()
        sent = xin.at[:, :, pl.ds(0, 14 * SEG)]
        pltpu.make_async_copy(sent, sent, send_in).wait()
        sent = obuf.at[:, :, pl.ds(0, 12 * SEG)]
        pltpu.make_async_copy(sent, sent, send_out).wait()

    pltpu.make_async_copy(ldin.at[pl.ds(0, 2 * (N - 1))], ldin.at[pl.ds(0, 2 * (N - 1))], send_ld).wait()


def _close(dqh, dkt, dvt, dq, dk, dv, dqt, sem):
    copies = [pltpu.make_async_copy(dkt, dk, sem.at[0]), pltpu.make_async_copy(dvt, dv, sem.at[1])]
    for copy in copies:
        copy.start()
    heads, tok = dqh.shape[:2]
    for g in range(heads // 8):
        part = pl.ds(g * 8, 8)
        _swap(dqt.at[g], dqh.at[part], tok, inverse=True)
        copies.append(pltpu.make_async_copy(dqt.at[g], dq.at[:, part], sem.at[2 + g]))
        copies[-1].start()
    for copy in copies:
        copy.wait()


def solution(mesh):
    spec = P('data', 'cp', None, None)
    lspec = P('data', None, 'cp')

    def local(q, k, v, o, lse, do):
        b, tok, heads, dim = q.shape
        hl = heads // N
        any_ = pl.BlockSpec(memory_space=pltpu.HBM)
        vmem = pl.BlockSpec(memory_space=pltpu.VMEM)
        seq = NSEG * SEG
        outs = pl.pallas_call(
            functools.partial(_kernel, hl, dim ** -0.5),
            out_shape=[jax.ShapeDtypeStruct((heads, tok, dim), BF16)] + [jax.ShapeDtypeStruct((tok, heads, dim), BF16)] * 2,
            in_specs=[any_] * 6,
            out_specs=[vmem] * 3,
            scratch_shapes=[
                pltpu.VMEM((RING, tok, 2 * hl, dim), BF16),
                pltpu.VMEM((heads, tok), F32),
                pltpu.VMEM((4, N // 2, 2 * hl, tok, dim), BF16),
                pltpu.VMEM((2 * hl, tok, dim), BF16),
                pltpu.VMEM((N // 2, 2, 2, 2 * hl, SEG), F32),
                pltpu.VMEM((hl, 4, seq, dim), BF16),
                pltpu.VMEM((NSEG, 2 * hl, SEG), F32),
                pltpu.VMEM((hl, 3, seq, dim), BF16),
                pltpu.VMEM((2, heads, tok, dim), BF16),
                pltpu.VMEM((seq, dim), F32),
                pltpu.VMEM((BLK, dim), F32),
                pltpu.VMEM((BLK, dim), F32),
                pltpu.VMEM((5, tok, dim), BF16),
                pltpu.VMEM((3, 4, hl, 2 * SEG, dim), BF16),
                pltpu.VMEM((3, 2, 2 * hl, SEG), F32),
                pltpu.VMEM((2, 3, hl, 2 * SEG, dim), BF16),
                pltpu.VMEM((3, hl, 2 * SEG, dim), F32),
                pltpu.VMEM((3, 2, hl - 1, SEG, dim), F32),
                pltpu.VMEM((3, 2, hl - 1, SEG, dim), F32),
                pltpu.VMEM((hl - 1, 2 * SEG, dim), F32),
                pltpu.VMEM((2 * SEG, dim), F32),
                pltpu.SemaphoreType.DMA((RING,)),
                pltpu.SemaphoreType.DMA,
                pltpu.SemaphoreType.DMA,
                pltpu.SemaphoreType.DMA((hl,)),
                pltpu.SemaphoreType.DMA,
                pltpu.SemaphoreType.DMA,
                pltpu.SemaphoreType.DMA,
                pltpu.SemaphoreType.DMA((3,)),
                pltpu.SemaphoreType.DMA,
                pltpu.SemaphoreType.DMA,
                pltpu.SemaphoreType.DMA((4,)),
                pltpu.SemaphoreType.DMA((2,)),
                pltpu.SemaphoreType.DMA,
                pltpu.SemaphoreType.DMA,
                pltpu.SemaphoreType.DMA,
                pltpu.SemaphoreType.DMA,
                pltpu.SemaphoreType.DMA,
            ],
            compiler_params=pltpu.CompilerParams(collective_id=0, has_side_effects=True,
                                                 vmem_limit_bytes=46 * 2 ** 20),
            name='attention_backward',
        )(q[0], k[0], v[0], do[0], o[0], lse[0])
        grads = pl.pallas_call(
            _close,
            out_shape=[jax.ShapeDtypeStruct((tok, heads, dim), BF16)] * 3,
            in_specs=[vmem] * 3,
            out_specs=[any_] * 3,
            scratch_shapes=[pltpu.VMEM((heads // 8, tok, 8, dim), BF16),
                            pltpu.SemaphoreType.DMA((2 + heads // 8,))],
            compiler_params=pltpu.CompilerParams(vmem_limit_bytes=16 * 2 ** 20),
            name='close',
        )(*outs)
        return tuple(x[None] for x in grads)

    return jax.shard_map(local, mesh=mesh, in_specs=(spec, spec, spec, spec, lspec, spec),
                         out_specs=(spec, spec, spec), check_vma=False)
```

```python
import functools

import jax
import jax.numpy as jnp
from jax import lax
from jax.experimental import pallas as pl
from jax.experimental.pallas import tpu as pltpu
from jax.sharding import PartitionSpec as P

F32 = jnp.float32
BF16 = jnp.bfloat16
MESH = pl.DeviceIdType.MESH
LOG2E = 1.4426950408889634

N = 8
SEG = 128
NSEG = 16
BLK = 512
CHIPS = ((0, 1), (1, 0), (1, 1), (0, 0))
CHUNK = 64
AHEAD = 4
RING = 6


def _chip(c, flips):
    fy, fx = flips
    if fy:
        c = (c + 2) % 4
    if fx:
        c = c + 1 - 2 * (c % 2)
    return c


def _nt(a, b):
    return lax.dot_general(a, b, (((1,), (1,)), ((), ())), preferred_element_type=F32)


def _tn(a, b):
    return lax.dot_general(a, b, (((0,), (0,)), ((), ())), preferred_element_type=F32)


def _nn(a, b):
    return lax.dot_general(a, b, (((1,), (0,)), ((), ())), preferred_element_type=F32)


def _swap(dst, src, tok, inverse=False):
    @pl.loop(0, tok // CHUNK)
    def _(i):
        r = pl.ds(pl.multiple_of(i * CHUNK, CHUNK), CHUNK)
        if inverse:
            dst[r] = jnp.swapaxes(src[:, r, :], 0, 1)
        else:
            dst[:, r, :] = jnp.swapaxes(src[r], 0, 1)


def _kernel(hl, scale, q, k, v, do, o, lse, dqh, dk, dv, nat, lsev, hm, ohm, ldst, xin, ldin, obuf, rin,
            dqacc, dkacc, dvacc, rel, loc, locld, lkv, ldq, gdq, rdq, fdq, pdq,
            nat_sem, lse_sem, send_in, recv_in, send_ld, recv_ld, send_out, recv_out,
            rel_sem, fwd_sem, send_loc, recv_loc, gdq_sem, send_fdq, rdq_sem, pdq_sem, send_pdq):
    me = lax.axis_index('cp')
    core = me % 2
    chip = me // 2
    chips = [_chip(chip, f) for f in CHIPS]
    tok = nat.shape[1]
    outer = chip != 0
    first = pl.ds(0, hl - 1)
    last = pl.ds((NSEG - 2) * SEG, 2 * SEG)
    peers = [[2 * chip + b for b in (0, 1)] for chip in chips]
    other = me + 1 - 2 * core
    remote = [p for c in (2, 1, 0) for p in peers[c]] + [other]

    barrier = pltpu.get_barrier_semaphore()
    for p in remote:
        pl.semaphore_signal(barrier, inc=1, device_id={'cp': p}, device_id_type=MESH)

    inputs = (q, k, v, do)
    group = [pl.ds(pl.multiple_of(chip * 2 * hl, 2 * hl), 2 * hl) for chip in chips]

    units = [(t, c) for t in range(4) for c in range(4)]
    loads = [pltpu.make_async_copy(x.at[:, group[c]], nat.at[(4 * t + c) % RING], nat_sem.at[(4 * t + c) % RING])
             for t, x in enumerate((*inputs, o)) for c in range(4)]
    for copy in loads[:AHEAD]:
        copy.start()
    load_lse = pltpu.make_async_copy(lse, lsev, lse_sem)
    load_lse.start()

    segs = (me, NSEG - 1 - me)
    rows = [pl.ds(pl.multiple_of(s * SEG, SEG), SEG) for s in segs]
    halves = [pl.ds(half * SEG, SEG) for half in (0, 1)]

    def send(t, c, h):
        for half in (0, 1):
            dst = xin.at[h, t, rows[half]]
            if c < 3:
                for b in (0, 1):
                    go = outer if t in (1, 2) and half == 1 else me >= 0
                    if c == 2 and h == hl - 1 and (t, b) in relayed:
                        go = jnp.logical_and(go, chip != 2)

                    @pl.when(go)
                    def _():
                        pltpu.make_async_remote_copy(hm.at[t, c, b * hl + h, halves[half]], dst, send_in, recv_in.at[h],
                                                     device_id={'cp': peers[c][b]}, device_id_type=MESH).start()
            else:
                pltpu.make_async_remote_copy(hm.at[t, c, (1 - core) * hl + h, halves[half]], dst, send_in, recv_in.at[h],
                                             device_id={'cp': other}, device_id_type=MESH).start()
                pltpu.make_async_copy(hm.at[t, c, core * hl + h, halves[half]], dst, recv_in.at[h]).start()

    relayed = [(0, 0), (0, 1), (1, 0), (1, 1), (2, 0)]

    def forward():
        pltpu.make_async_copy(rel, rel, rel_sem).wait()
        for n, (t, b) in enumerate(relayed):
            for half, seg in ((0, me + 4), (1, NSEG - 5 - me)):
                dst = xin.at[hl - 1, t, pl.ds(pl.multiple_of(seg * SEG, SEG), SEG)]
                pltpu.make_async_remote_copy(rel.at[n, halves[half]], dst, fwd_sem, recv_in.at[hl - 1],
                                             device_id={'cp': 2 + b}, device_id_type=MESH).start()

    @pl.when(outer)
    def _():
        for h in range(hl):
            for t in (1, 2):
                xin[h, t, last, :] = jnp.zeros((2 * SEG, xin.shape[-1]), BF16)

    for n, (t, c) in enumerate(units):
        if n + AHEAD < len(loads):
            loads[n + AHEAD].start()
        loads[n].wait()
        _swap(hm.at[t, c], nat.at[n % RING], tok)
        if n == 3:
            pl.semaphore_wait(barrier, N - 1)
            for unit in units[:n]:
                send(*unit, 0)
        elif n > 3:
            send(*units[n - 1], 0)

    row = lax.broadcasted_iota(jnp.int32, (2 * hl, nat.shape[-1]), 0)
    load_lse.wait()
    for c in range(4):
        loads[16 + c].wait()
        _swap(ohm, nat.at[(16 + c) % RING], tok)
        if c == 0:
            send(*units[-1], 0)
        delta = jnp.zeros((2 * hl, tok), F32)
        for g in range(2 * hl):
            prod = hm[3, c, g].astype(F32) * ohm[g].astype(F32)
            top = prod.astype(BF16)
            low = (prod - top.astype(F32)).astype(BF16)
            pick = jnp.where(row == g, 1.0, 0.0).astype(BF16)
            delta = delta + (_nt(pick, top) + _nt(pick, low))
        l2 = lsev[group[c], :] * LOG2E
        for b in (0, 1):
            for half in (0, 1):
                ldst[c, b, half, 0:hl, :] = l2[b * hl:(b + 1) * hl, half * SEG:(half + 1) * SEG]
                ldst[c, b, half, hl:2 * hl, :] = delta[b * hl:(b + 1) * hl, half * SEG:(half + 1) * SEG]
    for half in (0, 1):
        dst = ldin.at[segs[half]]
        for c in range(3):
            for b in (0, 1):
                pltpu.make_async_remote_copy(ldst.at[c, b, half], dst, send_ld, recv_ld,
                                             device_id={'cp': peers[c][b]}, device_id_type=MESH).start()
        pltpu.make_async_remote_copy(ldst.at[3, 1 - core, half], dst, send_ld, recv_ld,
                                     device_id={'cp': other}, device_id_type=MESH).start()
        pltpu.make_async_copy(ldst.at[3, core, half], dst, recv_ld).start()

    @pl.when(chip == 2)
    def _():
        for n, (t, b) in enumerate(relayed):
            pltpu.make_async_remote_copy(hm.at[t, 2, b * hl + hl - 1], rel.at[n], send_in, rel_sem,
                                         device_id={'cp': 2 * chips[1] + core}, device_id_type=MESH).start()

    own_rows = pl.ds(pl.multiple_of((1 - core) * SEG, SEG), SEG)
    other_rows = pl.ds(pl.multiple_of(core * SEG, SEG), SEG)
    own_heads = pl.ds(core * hl, hl)
    other_heads = pl.ds((1 - core) * hl, hl)

    @pl.when(chip == 0)
    def _():
        for c in range(3):
            for t in range(4):
                dst = loc.at[c, t, :, own_rows]
                pltpu.make_async_copy(hm.at[t, c, own_heads, halves[1]], dst, recv_loc.at[0]).start()
                pltpu.make_async_remote_copy(hm.at[t, c, other_heads, halves[1]], dst, send_loc.at[0], recv_loc.at[0],
                                             device_id={'cp': other}, device_id_type=MESH).start()
            dst = locld.at[c, 1 - core]
            pltpu.make_async_copy(ldst.at[c, core, 1], dst, recv_loc.at[1]).start()
            pltpu.make_async_remote_copy(ldst.at[c, 1 - core, 1], dst, send_loc.at[1], recv_loc.at[1],
                                         device_id={'cp': other}, device_id_type=MESH).start()

    for h in range(1, hl):
        for t in range(4):
            for c in (2, 1, 0, 3):
                send(t, c, h)

    @pl.when(chip == 0)
    def _():
        pltpu.make_async_copy(loc, loc, recv_loc.at[0]).wait()
        pltpu.make_async_copy(locld, locld, recv_loc.at[1]).wait()

        @pl.loop(0, 3 * hl)
        def _(i):
            c, h = i // hl, i % hl
            qb, kb, vb, dob = (loc[c, t, h] for t in range(4))
            l2 = jnp.concatenate([locld[c, s, pl.ds(h, 1), :] for s in (0, 1)], axis=1)
            dl = jnp.concatenate([locld[c, s, pl.ds(hl + h, 1), :] for s in (0, 1)], axis=1)
            p = jnp.exp2(_nt(kb, qb) * (scale * LOG2E) - l2)
            key = lax.broadcasted_iota(jnp.int32, p.shape, 0)
            query = lax.broadcasted_iota(jnp.int32, p.shape, 1)
            p = jnp.where(key <= query, p, 0.0)
            ds = (p * (_nt(vb, dob) - dl)).astype(BF16)
            lkv[0, c, h] = (_nn(ds, qb) * scale).astype(BF16)
            lkv[1, c, h] = _nn(p.astype(BF16), dob).astype(BF16)
            ldq[c, h] = _tn(ds, kb)

        for c in range(3):
            heads = pl.ds((2 * chips[c] + core) * hl, hl)
            for t in (0, 1):
                dst = rin.at[t, heads, halves[1]]
                pltpu.make_async_copy(lkv.at[t, c, :, own_rows], dst, recv_out.at[t + 1]).start()
                pltpu.make_async_remote_copy(lkv.at[t, c, :, other_rows], dst, send_loc.at[2], recv_out.at[t + 1],
                                             device_id={'cp': other}, device_id_type=MESH).start()
            dst = gdq.at[c, core]
            pltpu.make_async_copy(ldq.at[c, first, own_rows], dst, gdq_sem).start()
            pltpu.make_async_remote_copy(ldq.at[c, first, other_rows], dst, send_loc.at[3], gdq_sem,
                                         device_id={'cp': other}, device_id_type=MESH).start()
            pltpu.make_async_remote_copy(ldq.at[c, hl - 1], pdq, send_pdq, pdq_sem,
                                         device_id={'cp': peers[c][0] + core}, device_id_type=MESH).start()

    pltpu.make_async_copy(ldin, ldin, recv_ld).wait()

    nblk = NSEG * SEG // BLK
    per = BLK // SEG
    keys = jnp.where(outer, BLK - 2 * SEG, BLK)

    def head(h, carry):
        @pl.when(outer)
        def _():
            most = xin.at[h, :, pl.ds(0, (NSEG - 1) * SEG)]
            pltpu.make_async_copy(most, most, recv_in.at[h]).wait()

        @pl.when(chip == 0)
        def _():
            pltpu.make_async_copy(xin.at[h], xin.at[h], recv_in.at[h]).wait()

        dqacc[...] = jnp.zeros_like(dqacc)

        for j in range(nblk):
            kr = pl.ds(j * BLK, BLK)

            def tile(i, masked):
                qr = pl.ds(pl.multiple_of(i * BLK, BLK), BLK)
                qb, dob = xin[h, 0, qr, :], xin[h, 3, qr, :]
                kb, vb = xin[h, 1, kr, :], xin[h, 2, kr, :]
                l2 = jnp.concatenate([ldin[i * per + s, pl.ds(h, 1), :] for s in range(per)], axis=1)
                dl = jnp.concatenate([ldin[i * per + s, pl.ds(hl + h, 1), :] for s in range(per)], axis=1)
                p = jnp.exp2(_nt(kb, qb) * (scale * LOG2E) - l2)
                if masked:
                    key = lax.broadcasted_iota(jnp.int32, (BLK, BLK), 0)
                    query = lax.broadcasted_iota(jnp.int32, (BLK, BLK), 1)
                    seen = key <= query
                    if j == nblk - 1:
                        seen = jnp.logical_and(seen, key < keys)
                    p = jnp.where(seen, p, 0.0)
                ds = (p * (_nt(vb, dob) - dl)).astype(BF16)
                dvb = _nn(p.astype(BF16), dob)
                dkb = _nn(ds, qb)
                dqacc[qr, :] += _tn(ds, kb)
                return dkb, dvb

            dkb, dvb = tile(j, True)
            dkacc[...] = dkb
            dvacc[...] = dvb

            @pl.loop(j + 1, nblk)
            def _(i):
                dkb, dvb = tile(i, False)
                dkacc[...] += dkb
                dvacc[...] += dvb

            obuf[h, 1, kr, :] = (dkacc[...] * scale).astype(BF16)
            obuf[h, 2, kr, :] = dvacc[...].astype(BF16)

        @pl.when(jnp.logical_and(outer, h == hl - 1))
        def _():
            pltpu.make_async_copy(pdq, pdq, pdq_sem).wait()
            dqacc[last, :] += pdq[...]

        obuf[h, 0] = (dqacc[...] * scale).astype(BF16)

        @pl.when(jnp.logical_and(outer, h < hl - 1))
        def _():
            fdq[h] = dqacc[last, :]
            for b in (0, 1):
                pltpu.make_async_remote_copy(fdq.at[h, pl.ds((1 - b) * SEG, SEG)], rdq.at[chip - 1, core, h], send_fdq, rdq_sem,
                                             device_id={'cp': b}, device_id_type=MESH).start()

        @pl.when(jnp.logical_and(chip == 0, h == 0))
        def _():
            forward()

        mine = me * hl + h
        for t, x in ((1, rin.at[0]), (2, rin.at[1]), (0, dqh)):
            for p in remote:
                for half, seg in ((0, p), (1, NSEG - 1 - p)):
                    src = obuf.at[h, t, pl.ds(pl.multiple_of(seg * SEG, SEG), SEG)]
                    go = me >= 0
                    if half == 1:
                        go = jnp.logical_not(jnp.logical_and(outer, p < 2))

                    @pl.when(go)
                    def _():
                        pltpu.make_async_remote_copy(src, x.at[mine, halves[half]], send_out, recv_out.at[t],
                                                     device_id={'cp': p}, device_id_type=MESH).start()

                    if half == 1 and t == 0:
                        @pl.when(jnp.logical_and(jnp.logical_not(go), h == hl - 1))
                        def _():
                            pltpu.make_async_remote_copy(src, x.at[mine, halves[half]], send_pdq, recv_out.at[t],
                                                         device_id={'cp': p}, device_id_type=MESH).start()
            for half in (0, 1):
                pltpu.make_async_copy(obuf.at[h, t, rows[half]], x.at[mine, halves[half]], recv_out.at[t]).start()
        return carry

    lax.fori_loop(0, hl, head, 0)

    for t, x in ((1, dk), (2, dv)):
        src = rin.at[t - 1]
        pltpu.make_async_copy(src, src, recv_out.at[t]).wait()
        for g in range(N // 2):
            heads = pl.ds(g * 2 * hl, 2 * hl)
            _swap(x.at[:, heads], src.at[heads], tok, inverse=True)

    @pl.when(chip == 0)
    def _():
        pltpu.make_async_copy(gdq, gdq, gdq_sem).wait()
        pltpu.make_async_copy(rdq, rdq, rdq_sem).wait()

        few = hl - 1

        @pl.loop(0, 6 * few)
        def _(i):
            c, b, h = i // (2 * few), (i // few) % 2, i % few
            total = gdq[c, b, h] + rdq[c, b, h]
            dqh[(2 * c + 2 + b) * hl + h, halves[1], :] = (total * scale).astype(BF16)

        some = dqh.at[pl.ds(0, 2 * N * hl // 2 - 3 * few)]
        pltpu.make_async_copy(some, some, recv_out.at[0]).wait()
        pltpu.make_async_copy(ldq.at[:, hl - 1], ldq.at[:, hl - 1], send_pdq).wait()
        for n, ref in enumerate((loc.at[:, :, :, halves[0]], locld.at[:, 0], lkv.at[:, :, :, halves[0]], ldq.at[:, first, halves[0]])):
            pltpu.make_async_copy(ref, ref, send_loc.at[n]).wait()
        pltpu.make_async_copy(rel, rel, fwd_sem).wait()
        sent = xin.at[:, :, pl.ds(0, 11 * SEG)]
        pltpu.make_async_copy(sent, sent, send_in).wait()
        sent = obuf.at[:, :, pl.ds(0, 14 * SEG)]
        pltpu.make_async_copy(sent, sent, send_out).wait()

    @pl.when(outer)
    def _():
        pltpu.make_async_copy(dqh, dqh, recv_out.at[0]).wait()
        pltpu.make_async_copy(fdq, fdq, send_fdq).wait()
        sent = obuf.at[hl - 1, 0, last]
        pltpu.make_async_copy(sent, sent, send_pdq).wait()
        sent = xin.at[:, :, pl.ds(0, 14 * SEG)]
        pltpu.make_async_copy(sent, sent, send_in).wait()
        sent = obuf.at[:, :, pl.ds(0, 12 * SEG)]
        pltpu.make_async_copy(sent, sent, send_out).wait()

    pltpu.make_async_copy(ldin.at[pl.ds(0, 2 * (N - 1))], ldin.at[pl.ds(0, 2 * (N - 1))], send_ld).wait()


def _close(dqh, dkt, dvt, dq, dk, dv, dqt, sem):
    copies = [pltpu.make_async_copy(dkt, dk, sem.at[0]), pltpu.make_async_copy(dvt, dv, sem.at[1])]
    for copy in copies:
        copy.start()
    heads, tok = dqh.shape[:2]
    for g in range(heads // 8):
        part = pl.ds(g * 8, 8)
        _swap(dqt.at[g], dqh.at[part], tok, inverse=True)
        copies.append(pltpu.make_async_copy(dqt.at[g], dq.at[:, part], sem.at[2 + g]))
        copies[-1].start()
    for copy in copies:
        copy.wait()


def solution(mesh):
    spec = P('data', 'cp', None, None)
    lspec = P('data', None, 'cp')

    def local(q, k, v, o, lse, do):
        b, tok, heads, dim = q.shape
        hl = heads // N
        any_ = pl.BlockSpec(memory_space=pltpu.HBM)
        vmem = pl.BlockSpec(memory_space=pltpu.VMEM)
        seq = NSEG * SEG
        outs = pl.pallas_call(
            functools.partial(_kernel, hl, dim ** -0.5),
            out_shape=[jax.ShapeDtypeStruct((heads, tok, dim), BF16)] + [jax.ShapeDtypeStruct((tok, heads, dim), BF16)] * 2,
            in_specs=[any_] * 6,
            out_specs=[vmem] * 3,
            scratch_shapes=[
                pltpu.VMEM((RING, tok, 2 * hl, dim), BF16),
                pltpu.VMEM((heads, tok), F32),
                pltpu.VMEM((4, N // 2, 2 * hl, tok, dim), BF16),
                pltpu.VMEM((2 * hl, tok, dim), BF16),
                pltpu.VMEM((N // 2, 2, 2, 2 * hl, SEG), F32),
                pltpu.VMEM((hl, 4, seq, dim), BF16),
                pltpu.VMEM((NSEG, 2 * hl, SEG), F32),
                pltpu.VMEM((hl, 3, seq, dim), BF16),
                pltpu.VMEM((2, heads, tok, dim), BF16),
                pltpu.VMEM((seq, dim), F32),
                pltpu.VMEM((BLK, dim), F32),
                pltpu.VMEM((BLK, dim), F32),
                pltpu.VMEM((5, tok, dim), BF16),
                pltpu.VMEM((3, 4, hl, 2 * SEG, dim), BF16),
                pltpu.VMEM((3, 2, 2 * hl, SEG), F32),
                pltpu.VMEM((2, 3, hl, 2 * SEG, dim), BF16),
                pltpu.VMEM((3, hl, 2 * SEG, dim), F32),
                pltpu.VMEM((3, 2, hl - 1, SEG, dim), F32),
                pltpu.VMEM((3, 2, hl - 1, SEG, dim), F32),
                pltpu.VMEM((hl - 1, 2 * SEG, dim), F32),
                pltpu.VMEM((2 * SEG, dim), F32),
                pltpu.SemaphoreType.DMA((RING,)),
                pltpu.SemaphoreType.DMA,
                pltpu.SemaphoreType.DMA,
                pltpu.SemaphoreType.DMA((hl,)),
                pltpu.SemaphoreType.DMA,
                pltpu.SemaphoreType.DMA,
                pltpu.SemaphoreType.DMA,
                pltpu.SemaphoreType.DMA((3,)),
                pltpu.SemaphoreType.DMA,
                pltpu.SemaphoreType.DMA,
                pltpu.SemaphoreType.DMA((4,)),
                pltpu.SemaphoreType.DMA((2,)),
                pltpu.SemaphoreType.DMA,
                pltpu.SemaphoreType.DMA,
                pltpu.SemaphoreType.DMA,
                pltpu.SemaphoreType.DMA,
                pltpu.SemaphoreType.DMA,
            ],
            compiler_params=pltpu.CompilerParams(collective_id=0, has_side_effects=True,
                                                 vmem_limit_bytes=46 * 2 ** 20),
            name='attention_backward',
        )(q[0], k[0], v[0], do[0], o[0], lse[0])
        grads = pl.pallas_call(
            _close,
            out_shape=[jax.ShapeDtypeStruct((tok, heads, dim), BF16)] * 3,
            in_specs=[vmem] * 3,
            out_specs=[any_] * 3,
            scratch_shapes=[pltpu.VMEM((heads // 8, tok, 8, dim), BF16),
                            pltpu.SemaphoreType.DMA((2 + heads // 8,))],
            compiler_params=pltpu.CompilerParams(vmem_limit_bytes=16 * 2 ** 20),
            name='close',
        )(*outs)
        return tuple(x[None] for x in grads)

    return jax.shard_map(local, mesh=mesh, in_specs=(spec, spec, spec, spec, lspec, spec),
                         out_specs=(spec, spec, spec), check_vma=False)
```

```python
import functools

import jax
import jax.numpy as jnp
from jax import lax
from jax.experimental import pallas as pl
from jax.experimental.pallas import tpu as pltpu
from jax.sharding import PartitionSpec as P

F32 = jnp.float32
BF16 = jnp.bfloat16
MESH = pl.DeviceIdType.MESH
LOG2E = 1.4426950408889634

N = 8
SEG = 128
NSEG = 16
BLK = 512
CHIPS = ((0, 1), (1, 0), (1, 1), (0, 0))
CHUNK = 64
AHEAD = 4
RING = 6


def _chip(c, flips):
    fy, fx = flips
    if fy:
        c = (c + 2) % 4
    if fx:
        c = c + 1 - 2 * (c % 2)
    return c


def _nt(a, b):
    return lax.dot_general(a, b, (((1,), (1,)), ((), ())), preferred_element_type=F32)


def _tn(a, b):
    return lax.dot_general(a, b, (((0,), (0,)), ((), ())), preferred_element_type=F32)


def _nn(a, b):
    return lax.dot_general(a, b, (((1,), (0,)), ((), ())), preferred_element_type=F32)


def _swap(dst, src, tok, inverse=False):
    @pl.loop(0, tok // CHUNK)
    def _(i):
        r = pl.ds(pl.multiple_of(i * CHUNK, CHUNK), CHUNK)
        if inverse:
            dst[r] = jnp.swapaxes(src[:, r, :], 0, 1)
        else:
            dst[:, r, :] = jnp.swapaxes(src[r], 0, 1)


def _kernel(hl, scale, q, k, v, do, o, lse, dqh, dk, dv, nat, lsev, hm, ohm, ldst, xin, ldin, obuf, rin,
            dqacc, dkacc, dvacc, rel, loc, locld, lkv, ldq, gdq, rdq, fdq, pdq,
            nat_sem, lse_sem, send_in, recv_in, send_ld, recv_ld, send_out, recv_out,
            rel_sem, fwd_sem, send_loc, recv_loc, gdq_sem, send_fdq, rdq_sem, pdq_sem, send_pdq):
    me = lax.axis_index('cp')
    core = me % 2
    chip = me // 2
    chips = [_chip(chip, f) for f in CHIPS]
    tok = nat.shape[1]
    outer = chip != 0
    first = pl.ds(0, hl - 1)
    last = pl.ds((NSEG - 2) * SEG, 2 * SEG)
    peers = [[2 * chip + b for b in (0, 1)] for chip in chips]
    other = me + 1 - 2 * core
    remote = [p for c in (2, 1, 0) for p in peers[c]] + [other]

    barrier = pltpu.get_barrier_semaphore()
    for p in remote:
        pl.semaphore_signal(barrier, inc=1, device_id={'cp': p}, device_id_type=MESH)

    inputs = (q, k, v, do)
    group = [pl.ds(pl.multiple_of(chip * 2 * hl, 2 * hl), 2 * hl) for chip in chips]

    units = [(t, c) for t in range(4) for c in range(4)]
    loads = [pltpu.make_async_copy(x.at[:, group[c]], nat.at[(4 * t + c) % RING], nat_sem.at[(4 * t + c) % RING])
             for t, x in enumerate((*inputs, o)) for c in range(4)]
    for copy in loads[:AHEAD]:
        copy.start()
    load_lse = pltpu.make_async_copy(lse, lsev, lse_sem)
    load_lse.start()

    segs = (me, NSEG - 1 - me)
    rows = [pl.ds(pl.multiple_of(s * SEG, SEG), SEG) for s in segs]
    halves = [pl.ds(half * SEG, SEG) for half in (0, 1)]

    def send(t, c, h):
        for half in (0, 1):
            dst = xin.at[h, t, rows[half]]
            if c < 3:
                for b in (0, 1):
                    go = outer if t in (1, 2) and half == 1 else me >= 0
                    if c == 2 and h == hl - 1 and (t, b) in relayed:
                        go = jnp.logical_and(go, chip != 2)

                    @pl.when(go)
                    def _():
                        pltpu.make_async_remote_copy(hm.at[t, c, b * hl + h, halves[half]], dst, send_in, recv_in.at[h],
                                                     device_id={'cp': peers[c][b]}, device_id_type=MESH).start()
            else:
                pltpu.make_async_remote_copy(hm.at[t, c, (1 - core) * hl + h, halves[half]], dst, send_in, recv_in.at[h],
                                             device_id={'cp': other}, device_id_type=MESH).start()
                pltpu.make_async_copy(hm.at[t, c, core * hl + h, halves[half]], dst, recv_in.at[h]).start()

    relayed = [(0, 0), (0, 1), (1, 0), (1, 1), (2, 0)]

    def forward():
        pltpu.make_async_copy(rel, rel, rel_sem).wait()
        for n, (t, b) in enumerate(relayed):
            for half, seg in ((0, me + 4), (1, NSEG - 5 - me)):
                dst = xin.at[hl - 1, t, pl.ds(pl.multiple_of(seg * SEG, SEG), SEG)]
                pltpu.make_async_remote_copy(rel.at[n, halves[half]], dst, fwd_sem, recv_in.at[hl - 1],
                                             device_id={'cp': 2 + b}, device_id_type=MESH).start()

    @pl.when(outer)
    def _():
        for h in range(hl):
            for t in (1, 2):
                xin[h, t, last, :] = jnp.zeros((2 * SEG, xin.shape[-1]), BF16)

    for n, (t, c) in enumerate(units):
        if n + AHEAD < len(loads):
            loads[n + AHEAD].start()
        loads[n].wait()
        _swap(hm.at[t, c], nat.at[n % RING], tok)
        if n == 3:
            pl.semaphore_wait(barrier, N - 1)
            for unit in units[:n]:
                send(*unit, 0)
        elif n > 3:
            send(*units[n - 1], 0)

    row = lax.broadcasted_iota(jnp.int32, (2 * hl, nat.shape[-1]), 0)
    load_lse.wait()
    for c in range(4):
        loads[16 + c].wait()
        _swap(ohm, nat.at[(16 + c) % RING], tok)
        if c == 0:
            send(*units[-1], 0)
        delta = jnp.zeros((2 * hl, tok), F32)
        for g in range(2 * hl):
            prod = (0.5 * hm[3, c, g].astype(F32)) * ohm[g].astype(F32)
            top = prod.astype(BF16)
            low = (prod - top.astype(F32)).astype(BF16)
            pick = jnp.where(row == g, 1.0, 0.0).astype(BF16)
            delta = delta + (_nt(pick, top) + _nt(pick, low))
        l2 = lsev[group[c], :] * LOG2E
        for b in (0, 1):
            for half in (0, 1):
                ldst[c, b, half, 0:hl, :] = l2[b * hl:(b + 1) * hl, half * SEG:(half + 1) * SEG]
                ldst[c, b, half, hl:2 * hl, :] = 2.0 * delta[b * hl:(b + 1) * hl, half * SEG:(half + 1) * SEG]
    for half in (0, 1):
        dst = ldin.at[segs[half]]
        for c in range(3):
            for b in (0, 1):
                pltpu.make_async_remote_copy(ldst.at[c, b, half], dst, send_ld, recv_ld,
                                             device_id={'cp': peers[c][b]}, device_id_type=MESH).start()
        pltpu.make_async_remote_copy(ldst.at[3, 1 - core, half], dst, send_ld, recv_ld,
                                     device_id={'cp': other}, device_id_type=MESH).start()
        pltpu.make_async_copy(ldst.at[3, core, half], dst, recv_ld).start()

    @pl.when(chip == 2)
    def _():
        for n, (t, b) in enumerate(relayed):
            pltpu.make_async_remote_copy(hm.at[t, 2, b * hl + hl - 1], rel.at[n], send_in, rel_sem,
                                         device_id={'cp': 2 * chips[1] + core}, device_id_type=MESH).start()

    own_rows = pl.ds(pl.multiple_of((1 - core) * SEG, SEG), SEG)
    other_rows = pl.ds(pl.multiple_of(core * SEG, SEG), SEG)
    own_heads = pl.ds(core * hl, hl)
    other_heads = pl.ds((1 - core) * hl, hl)

    @pl.when(chip == 0)
    def _():
        for c in range(3):
            for t in range(4):
                dst = loc.at[c, t, :, own_rows]
                pltpu.make_async_copy(hm.at[t, c, own_heads, halves[1]], dst, recv_loc.at[0]).start()
                pltpu.make_async_remote_copy(hm.at[t, c, other_heads, halves[1]], dst, send_loc.at[0], recv_loc.at[0],
                                             device_id={'cp': other}, device_id_type=MESH).start()
            dst = locld.at[c, 1 - core]
            pltpu.make_async_copy(ldst.at[c, core, 1], dst, recv_loc.at[1]).start()
            pltpu.make_async_remote_copy(ldst.at[c, 1 - core, 1], dst, send_loc.at[1], recv_loc.at[1],
                                         device_id={'cp': other}, device_id_type=MESH).start()

    for h in range(1, hl):
        for t in range(4):
            for c in (2, 1, 0, 3):
                send(t, c, h)

    @pl.when(chip == 0)
    def _():
        pltpu.make_async_copy(loc, loc, recv_loc.at[0]).wait()
        pltpu.make_async_copy(locld, locld, recv_loc.at[1]).wait()

        @pl.loop(0, 3 * hl)
        def _(i):
            c, h = i // hl, i % hl
            qb, kb, vb, dob = (loc[c, t, h] for t in range(4))
            l2 = jnp.concatenate([locld[c, s, pl.ds(h, 1), :] for s in (0, 1)], axis=1)
            dl = jnp.concatenate([locld[c, s, pl.ds(hl + h, 1), :] for s in (0, 1)], axis=1)
            p = jnp.exp2(_nt(kb, qb) * (scale * LOG2E) - l2)
            key = lax.broadcasted_iota(jnp.int32, p.shape, 0)
            query = lax.broadcasted_iota(jnp.int32, p.shape, 1)
            p = jnp.where(key <= query, p, 0.0)
            ds = (p * (_nt(vb, dob) - dl)).astype(BF16)
            lkv[0, c, h] = (_nn(ds, qb) * scale).astype(BF16)
            lkv[1, c, h] = _nn(p.astype(BF16), dob).astype(BF16)
            ldq[c, h] = _tn(ds, kb)

        for c in range(3):
            heads = pl.ds((2 * chips[c] + core) * hl, hl)
            for t in (0, 1):
                dst = rin.at[t, heads, halves[1]]
                pltpu.make_async_copy(lkv.at[t, c, :, own_rows], dst, recv_out.at[t + 1]).start()
                pltpu.make_async_remote_copy(lkv.at[t, c, :, other_rows], dst, send_loc.at[2], recv_out.at[t + 1],
                                             device_id={'cp': other}, device_id_type=MESH).start()
            dst = gdq.at[c, core]
            pltpu.make_async_copy(ldq.at[c, first, own_rows], dst, gdq_sem).start()
            pltpu.make_async_remote_copy(ldq.at[c, first, other_rows], dst, send_loc.at[3], gdq_sem,
                                         device_id={'cp': other}, device_id_type=MESH).start()
            pltpu.make_async_remote_copy(ldq.at[c, hl - 1], pdq, send_pdq, pdq_sem,
                                         device_id={'cp': peers[c][0] + core}, device_id_type=MESH).start()

    pltpu.make_async_copy(ldin, ldin, recv_ld).wait()

    nblk = NSEG * SEG // BLK
    per = BLK // SEG
    keys = jnp.where(outer, BLK - 2 * SEG, BLK)

    def head(h, carry):
        @pl.when(outer)
        def _():
            most = xin.at[h, :, pl.ds(0, (NSEG - 1) * SEG)]
            pltpu.make_async_copy(most, most, recv_in.at[h]).wait()

        @pl.when(chip == 0)
        def _():
            pltpu.make_async_copy(xin.at[h], xin.at[h], recv_in.at[h]).wait()

        dqacc[...] = jnp.zeros_like(dqacc)

        for j in range(nblk):
            kr = pl.ds(j * BLK, BLK)

            def tile(i, masked):
                qr = pl.ds(pl.multiple_of(i * BLK, BLK), BLK)
                qb, dob = xin[h, 0, qr, :], xin[h, 3, qr, :]
                kb, vb = xin[h, 1, kr, :], xin[h, 2, kr, :]
                l2 = jnp.concatenate([ldin[i * per + s, pl.ds(h, 1), :] for s in range(per)], axis=1)
                dl = jnp.concatenate([ldin[i * per + s, pl.ds(hl + h, 1), :] for s in range(per)], axis=1)
                p = jnp.exp2(_nt(kb, qb) * (scale * LOG2E) - l2)
                if masked:
                    key = lax.broadcasted_iota(jnp.int32, (BLK, BLK), 0)
                    query = lax.broadcasted_iota(jnp.int32, (BLK, BLK), 1)
                    seen = key <= query
                    if j == nblk - 1:
                        seen = jnp.logical_and(seen, key < keys)
                    p = jnp.where(seen, p, 0.0)
                ds = (p * (_nt(vb, dob) - dl)).astype(BF16)
                dvb = _nn(p.astype(BF16), dob)
                dkb = _nn(ds, qb)
                dqacc[qr, :] += _tn(ds, kb)
                return dkb, dvb

            dkb, dvb = tile(j, True)
            dkacc[...] = dkb
            dvacc[...] = dvb

            @pl.loop(j + 1, nblk)
            def _(i):
                dkb, dvb = tile(i, False)
                dkacc[...] += dkb
                dvacc[...] += dvb

            obuf[h, 1, kr, :] = (dkacc[...] * scale).astype(BF16)
            obuf[h, 2, kr, :] = dvacc[...].astype(BF16)

        @pl.when(jnp.logical_and(outer, h == hl - 1))
        def _():
            pltpu.make_async_copy(pdq, pdq, pdq_sem).wait()
            dqacc[last, :] += pdq[...]

        obuf[h, 0] = (dqacc[...] * scale).astype(BF16)

        @pl.when(jnp.logical_and(outer, h < hl - 1))
        def _():
            fdq[h] = dqacc[last, :]
            for b in (0, 1):
                pltpu.make_async_remote_copy(fdq.at[h, pl.ds((1 - b) * SEG, SEG)], rdq.at[chip - 1, core, h], send_fdq, rdq_sem,
                                             device_id={'cp': b}, device_id_type=MESH).start()

        @pl.when(jnp.logical_and(chip == 0, h == 0))
        def _():
            forward()

        mine = me * hl + h
        for t, x in ((1, rin.at[0]), (2, rin.at[1]), (0, dqh)):
            for p in remote:
                for half, seg in ((0, p), (1, NSEG - 1 - p)):
                    src = obuf.at[h, t, pl.ds(pl.multiple_of(seg * SEG, SEG), SEG)]
                    go = me >= 0
                    if half == 1:
                        go = jnp.logical_not(jnp.logical_and(outer, p < 2))

                    @pl.when(go)
                    def _():
                        pltpu.make_async_remote_copy(src, x.at[mine, halves[half]], send_out, recv_out.at[t],
                                                     device_id={'cp': p}, device_id_type=MESH).start()

                    if half == 1 and t == 0:
                        @pl.when(jnp.logical_and(jnp.logical_not(go), h == hl - 1))
                        def _():
                            pltpu.make_async_remote_copy(src, x.at[mine, halves[half]], send_pdq, recv_out.at[t],
                                                         device_id={'cp': p}, device_id_type=MESH).start()
            for half in (0, 1):
                pltpu.make_async_copy(obuf.at[h, t, rows[half]], x.at[mine, halves[half]], recv_out.at[t]).start()
        return carry

    lax.fori_loop(0, hl, head, 0)

    for t, x in ((1, dk), (2, dv)):
        src = rin.at[t - 1]
        pltpu.make_async_copy(src, src, recv_out.at[t]).wait()
        for g in range(N // 2):
            heads = pl.ds(g * 2 * hl, 2 * hl)
            _swap(x.at[:, heads], src.at[heads], tok, inverse=True)

    @pl.when(chip == 0)
    def _():
        pltpu.make_async_copy(gdq, gdq, gdq_sem).wait()
        pltpu.make_async_copy(rdq, rdq, rdq_sem).wait()

        few = hl - 1

        @pl.loop(0, 6 * few)
        def _(i):
            c, b, h = i // (2 * few), (i // few) % 2, i % few
            total = gdq[c, b, h] + rdq[c, b, h]
            dqh[(2 * c + 2 + b) * hl + h, halves[1], :] = (total * scale).astype(BF16)

        some = dqh.at[pl.ds(0, 2 * N * hl // 2 - 3 * few)]
        pltpu.make_async_copy(some, some, recv_out.at[0]).wait()
        pltpu.make_async_copy(ldq.at[:, hl - 1], ldq.at[:, hl - 1], send_pdq).wait()
        for n, ref in enumerate((loc.at[:, :, :, halves[0]], locld.at[:, 0], lkv.at[:, :, :, halves[0]], ldq.at[:, first, halves[0]])):
            pltpu.make_async_copy(ref, ref, send_loc.at[n]).wait()
        pltpu.make_async_copy(rel, rel, fwd_sem).wait()
        sent = xin.at[:, :, pl.ds(0, 11 * SEG)]
        pltpu.make_async_copy(sent, sent, send_in).wait()
        sent = obuf.at[:, :, pl.ds(0, 14 * SEG)]
        pltpu.make_async_copy(sent, sent, send_out).wait()

    @pl.when(outer)
    def _():
        pltpu.make_async_copy(dqh, dqh, recv_out.at[0]).wait()
        pltpu.make_async_copy(fdq, fdq, send_fdq).wait()
        sent = obuf.at[hl - 1, 0, last]
        pltpu.make_async_copy(sent, sent, send_pdq).wait()
        sent = xin.at[:, :, pl.ds(0, 14 * SEG)]
        pltpu.make_async_copy(sent, sent, send_in).wait()
        sent = obuf.at[:, :, pl.ds(0, 12 * SEG)]
        pltpu.make_async_copy(sent, sent, send_out).wait()

    pltpu.make_async_copy(ldin.at[pl.ds(0, 2 * (N - 1))], ldin.at[pl.ds(0, 2 * (N - 1))], send_ld).wait()


def _close(dqh, dkt, dvt, dq, dk, dv, dqt, sem):
    copies = [pltpu.make_async_copy(dkt, dk, sem.at[0]), pltpu.make_async_copy(dvt, dv, sem.at[1])]
    for copy in copies:
        copy.start()
    heads, tok = dqh.shape[:2]
    for g in range(heads // 8):
        part = pl.ds(g * 8, 8)
        _swap(dqt.at[g], dqh.at[part], tok, inverse=True)
        copies.append(pltpu.make_async_copy(dqt.at[g], dq.at[:, part], sem.at[2 + g]))
        copies[-1].start()
    for copy in copies:
        copy.wait()


def solution(mesh):
    spec = P('data', 'cp', None, None)
    lspec = P('data', None, 'cp')

    def local(q, k, v, o, lse, do):
        b, tok, heads, dim = q.shape
        hl = heads // N
        any_ = pl.BlockSpec(memory_space=pltpu.HBM)
        vmem = pl.BlockSpec(memory_space=pltpu.VMEM)
        seq = NSEG * SEG
        outs = pl.pallas_call(
            functools.partial(_kernel, hl, dim ** -0.5),
            out_shape=[jax.ShapeDtypeStruct((heads, tok, dim), BF16)] + [jax.ShapeDtypeStruct((tok, heads, dim), BF16)] * 2,
            in_specs=[any_] * 6,
            out_specs=[vmem] * 3,
            scratch_shapes=[
                pltpu.VMEM((RING, tok, 2 * hl, dim), BF16),
                pltpu.VMEM((heads, tok), F32),
                pltpu.VMEM((4, N // 2, 2 * hl, tok, dim), BF16),
                pltpu.VMEM((2 * hl, tok, dim), BF16),
                pltpu.VMEM((N // 2, 2, 2, 2 * hl, SEG), F32),
                pltpu.VMEM((hl, 4, seq, dim), BF16),
                pltpu.VMEM((NSEG, 2 * hl, SEG), F32),
                pltpu.VMEM((hl, 3, seq, dim), BF16),
                pltpu.VMEM((2, heads, tok, dim), BF16),
                pltpu.VMEM((seq, dim), F32),
                pltpu.VMEM((BLK, dim), F32),
                pltpu.VMEM((BLK, dim), F32),
                pltpu.VMEM((5, tok, dim), BF16),
                pltpu.VMEM((3, 4, hl, 2 * SEG, dim), BF16),
                pltpu.VMEM((3, 2, 2 * hl, SEG), F32),
                pltpu.VMEM((2, 3, hl, 2 * SEG, dim), BF16),
                pltpu.VMEM((3, hl, 2 * SEG, dim), F32),
                pltpu.VMEM((3, 2, hl - 1, SEG, dim), F32),
                pltpu.VMEM((3, 2, hl - 1, SEG, dim), F32),
                pltpu.VMEM((hl - 1, 2 * SEG, dim), F32),
                pltpu.VMEM((2 * SEG, dim), F32),
                pltpu.SemaphoreType.DMA((RING,)),
                pltpu.SemaphoreType.DMA,
                pltpu.SemaphoreType.DMA,
                pltpu.SemaphoreType.DMA((hl,)),
                pltpu.SemaphoreType.DMA,
                pltpu.SemaphoreType.DMA,
                pltpu.SemaphoreType.DMA,
                pltpu.SemaphoreType.DMA((3,)),
                pltpu.SemaphoreType.DMA,
                pltpu.SemaphoreType.DMA,
                pltpu.SemaphoreType.DMA((4,)),
                pltpu.SemaphoreType.DMA((2,)),
                pltpu.SemaphoreType.DMA,
                pltpu.SemaphoreType.DMA,
                pltpu.SemaphoreType.DMA,
                pltpu.SemaphoreType.DMA,
                pltpu.SemaphoreType.DMA,
            ],
            compiler_params=pltpu.CompilerParams(collective_id=0, has_side_effects=True,
                                                 vmem_limit_bytes=46 * 2 ** 20),
            name='attention_backward',
        )(q[0], k[0], v[0], do[0], o[0], lse[0])
        grads = pl.pallas_call(
            _close,
            out_shape=[jax.ShapeDtypeStruct((tok, heads, dim), BF16)] * 3,
            in_specs=[vmem] * 3,
            out_specs=[any_] * 3,
            scratch_shapes=[pltpu.VMEM((heads // 8, tok, 8, dim), BF16),
                            pltpu.SemaphoreType.DMA((2 + heads // 8,))],
            compiler_params=pltpu.CompilerParams(vmem_limit_bytes=16 * 2 ** 20),
            name='close',
        )(*outs)
        return tuple(x[None] for x in grads)

    return jax.shard_map(local, mesh=mesh, in_specs=(spec, spec, spec, spec, lspec, spec),
                         out_specs=(spec, spec, spec), check_vma=False)
```

```python
import functools

import jax
import jax.numpy as jnp
from jax import lax
from jax.experimental import pallas as pl
from jax.experimental.pallas import tpu as pltpu
from jax.sharding import PartitionSpec as P

F32 = jnp.float32
BF16 = jnp.bfloat16
MESH = pl.DeviceIdType.MESH
LOG2E = 1.4426950408889634

N = 8
SEG = 128
NSEG = 16
BLK = 512
CHIPS = ((0, 1), (1, 0), (1, 1), (0, 0))
CHUNK = 64
AHEAD = 4
RING = 6


def _chip(c, flips):
    fy, fx = flips
    if fy:
        c = (c + 2) % 4
    if fx:
        c = c + 1 - 2 * (c % 2)
    return c


def _nt(a, b):
    return lax.dot_general(a, b, (((1,), (1,)), ((), ())), preferred_element_type=F32)


def _tn(a, b):
    return lax.dot_general(a, b, (((0,), (0,)), ((), ())), preferred_element_type=F32)


def _nn(a, b):
    return lax.dot_general(a, b, (((1,), (0,)), ((), ())), preferred_element_type=F32)


def _swap(dst, src, tok, inverse=False):
    @pl.loop(0, tok // CHUNK)
    def _(i):
        r = pl.ds(pl.multiple_of(i * CHUNK, CHUNK), CHUNK)
        if inverse:
            dst[r] = jnp.swapaxes(src[:, r, :], 0, 1)
        else:
            dst[:, r, :] = jnp.swapaxes(src[r], 0, 1)


def _kernel(hl, scale, q, k, v, do, o, lse, dqh, dk, dv, nat, lsev, hm, ohm, ldst, xin, ldin, obuf, rin,
            dqacc, dkacc, dvacc, rel, loc, locld, lkv, ldq, gdq, rdq, fdq, pdq,
            nat_sem, lse_sem, send_in, recv_in, send_ld, recv_ld, send_out, recv_out,
            rel_sem, fwd_sem, send_loc, recv_loc, gdq_sem, send_fdq, rdq_sem, pdq_sem, send_pdq):
    me = lax.axis_index('cp')
    core = me % 2
    chip = me // 2
    chips = [_chip(chip, f) for f in CHIPS]
    tok = nat.shape[1]
    outer = chip != 0
    first = pl.ds(0, hl - 1)
    last = pl.ds((NSEG - 2) * SEG, 2 * SEG)
    peers = [[2 * chip + b for b in (0, 1)] for chip in chips]
    other = me + 1 - 2 * core
    remote = [p for c in (2, 1, 0) for p in peers[c]] + [other]

    barrier = pltpu.get_barrier_semaphore()
    for p in remote:
        pl.semaphore_signal(barrier, inc=1, device_id={'cp': p}, device_id_type=MESH)

    inputs = (q, k, v, do)
    group = [pl.ds(pl.multiple_of(chip * 2 * hl, 2 * hl), 2 * hl) for chip in chips]

    units = [(t, c) for t in range(4) for c in range(4)]
    loads = [pltpu.make_async_copy(x.at[:, group[c]], nat.at[(4 * t + c) % RING], nat_sem.at[(4 * t + c) % RING])
             for t, x in enumerate((*inputs, o)) for c in range(4)]
    for copy in loads[:AHEAD]:
        copy.start()
    load_lse = pltpu.make_async_copy(lse, lsev, lse_sem)
    load_lse.start()

    segs = (me, NSEG - 1 - me)
    rows = [pl.ds(pl.multiple_of(s * SEG, SEG), SEG) for s in segs]
    halves = [pl.ds(half * SEG, SEG) for half in (0, 1)]

    def send(t, c, h):
        for half in (0, 1):
            dst = xin.at[h, t, rows[half]]
            if c < 3:
                for b in (0, 1):
                    go = outer if t in (1, 2) and half == 1 else me >= 0
                    if c == 2 and h == hl - 1 and (t, b) in relayed:
                        go = jnp.logical_and(go, chip != 2)

                    @pl.when(go)
                    def _():
                        pltpu.make_async_remote_copy(hm.at[t, c, b * hl + h, halves[half]], dst, send_in, recv_in.at[h],
                                                     device_id={'cp': peers[c][b]}, device_id_type=MESH).start()
            else:
                pltpu.make_async_remote_copy(hm.at[t, c, (1 - core) * hl + h, halves[half]], dst, send_in, recv_in.at[h],
                                             device_id={'cp': other}, device_id_type=MESH).start()
                pltpu.make_async_copy(hm.at[t, c, core * hl + h, halves[half]], dst, recv_in.at[h]).start()

    relayed = [(0, 0), (0, 1), (1, 0), (1, 1), (2, 0)]

    def forward():
        pltpu.make_async_copy(rel, rel, rel_sem).wait()
        for n, (t, b) in enumerate(relayed):
            for half, seg in ((0, me + 4), (1, NSEG - 5 - me)):
                dst = xin.at[hl - 1, t, pl.ds(pl.multiple_of(seg * SEG, SEG), SEG)]
                pltpu.make_async_remote_copy(rel.at[n, halves[half]], dst, fwd_sem, recv_in.at[hl - 1],
                                             device_id={'cp': 2 + b}, device_id_type=MESH).start()

    @pl.when(outer)
    def _():
        for h in range(hl):
            for t in (1, 2):
                xin[h, t, last, :] = jnp.zeros((2 * SEG, xin.shape[-1]), BF16)

    for n, (t, c) in enumerate(units):
        if n + AHEAD < len(loads):
            loads[n + AHEAD].start()
        loads[n].wait()
        _swap(hm.at[t, c], nat.at[n % RING], tok)
        if n == 3:
            pl.semaphore_wait(barrier, N - 1)
            for unit in units[:n]:
                send(*unit, 0)
        elif n > 3:
            send(*units[n - 1], 0)

    row = lax.broadcasted_iota(jnp.int32, (2 * hl, nat.shape[-1]), 0)
    load_lse.wait()
    for c in range(4):
        loads[16 + c].wait()
        _swap(ohm, nat.at[(16 + c) % RING], tok)
        if c == 0:
            send(*units[-1], 0)
        delta = jnp.zeros((2 * hl, tok), F32)
        for g in range(2 * hl):
            prod = (0.5 * hm[3, c, g].astype(F32)) * ohm[g].astype(F32)
            top = prod.astype(BF16)
            low = (prod - top.astype(F32)).astype(BF16)
            pick = jnp.where(row == g, 1.0, 0.0).astype(BF16)
            delta = delta + (_nt(pick, top) + _nt(pick, low))
        l2 = lsev[group[c], :] * LOG2E
        for b in (0, 1):
            for half in (0, 1):
                ldst[c, b, half, 0:hl, :] = l2[b * hl:(b + 1) * hl, half * SEG:(half + 1) * SEG]
                ldst[c, b, half, hl:2 * hl, :] = 2.0 * delta[b * hl:(b + 1) * hl, half * SEG:(half + 1) * SEG]
    for half in (0, 1):
        dst = ldin.at[segs[half]]
        for c in range(3):
            for b in (0, 1):
                pltpu.make_async_remote_copy(ldst.at[c, b, half], dst, send_ld, recv_ld,
                                             device_id={'cp': peers[c][b]}, device_id_type=MESH).start()
        pltpu.make_async_remote_copy(ldst.at[3, 1 - core, half], dst, send_ld, recv_ld,
                                     device_id={'cp': other}, device_id_type=MESH).start()
        pltpu.make_async_copy(ldst.at[3, core, half], dst, recv_ld).start()

    @pl.when(chip == 2)
    def _():
        for n, (t, b) in enumerate(relayed):
            pltpu.make_async_remote_copy(hm.at[t, 2, b * hl + hl - 1], rel.at[n], send_in, rel_sem,
                                         device_id={'cp': 2 * chips[1] + core}, device_id_type=MESH).start()

    own_rows = pl.ds(pl.multiple_of((1 - core) * SEG, SEG), SEG)
    other_rows = pl.ds(pl.multiple_of(core * SEG, SEG), SEG)
    own_heads = pl.ds(core * hl, hl)
    other_heads = pl.ds((1 - core) * hl, hl)

    @pl.when(chip == 0)
    def _():
        for c in range(3):
            for t in range(4):
                dst = loc.at[c, t, :, own_rows]
                pltpu.make_async_copy(hm.at[t, c, own_heads, halves[1]], dst, recv_loc.at[0]).start()
                pltpu.make_async_remote_copy(hm.at[t, c, other_heads, halves[1]], dst, send_loc.at[0], recv_loc.at[0],
                                             device_id={'cp': other}, device_id_type=MESH).start()
            dst = locld.at[c, 1 - core]
            pltpu.make_async_copy(ldst.at[c, core, 1], dst, recv_loc.at[1]).start()
            pltpu.make_async_remote_copy(ldst.at[c, 1 - core, 1], dst, send_loc.at[1], recv_loc.at[1],
                                         device_id={'cp': other}, device_id_type=MESH).start()

    for h in range(1, hl):
        for t in range(4):
            for c in (2, 1, 0, 3):
                send(t, c, h)

    @pl.when(chip == 0)
    def _():
        pltpu.make_async_copy(loc, loc, recv_loc.at[0]).wait()
        pltpu.make_async_copy(locld, locld, recv_loc.at[1]).wait()

        @pl.loop(0, 3 * hl)
        def _(i):
            c, h = i // hl, i % hl
            qb, kb, vb, dob = (loc[c, t, h] for t in range(4))
            l2 = jnp.concatenate([locld[c, s, pl.ds(h, 1), :] for s in (0, 1)], axis=1)
            dl = jnp.concatenate([locld[c, s, pl.ds(hl + h, 1), :] for s in (0, 1)], axis=1)
            p = jnp.exp2(_nt(kb, qb) * (scale * LOG2E) - l2)
            key = lax.broadcasted_iota(jnp.int32, p.shape, 0)
            query = lax.broadcasted_iota(jnp.int32, p.shape, 1)
            p = jnp.where(key <= query, p, 0.0)
            ds = (p * (_nt(vb, dob) - dl)).astype(BF16)
            lkv[0, c, h] = (_nn(ds, qb) * scale).astype(BF16)
            lkv[1, c, h] = _nn(p.astype(BF16), dob).astype(BF16)
            ldq[c, h] = _tn(ds, kb)

        for c in range(3):
            heads = pl.ds((2 * chips[c] + core) * hl, hl)
            for t in (0, 1):
                dst = rin.at[t, heads, halves[1]]
                pltpu.make_async_copy(lkv.at[t, c, :, own_rows], dst, recv_out.at[t + 1]).start()
                pltpu.make_async_remote_copy(lkv.at[t, c, :, other_rows], dst, send_loc.at[2], recv_out.at[t + 1],
                                             device_id={'cp': other}, device_id_type=MESH).start()
            dst = gdq.at[c, core]
            pltpu.make_async_copy(ldq.at[c, first, own_rows], dst, gdq_sem).start()
            pltpu.make_async_remote_copy(ldq.at[c, first, other_rows], dst, send_loc.at[3], gdq_sem,
                                         device_id={'cp': other}, device_id_type=MESH).start()
            pltpu.make_async_remote_copy(ldq.at[c, hl - 1], pdq, send_pdq, pdq_sem,
                                         device_id={'cp': peers[c][0] + core}, device_id_type=MESH).start()

    pltpu.make_async_copy(ldin, ldin, recv_ld).wait()

    nblk = NSEG * SEG // BLK
    per = BLK // SEG
    keys = jnp.where(outer, BLK - 2 * SEG, BLK)

    def head(h, carry):
        @pl.when(outer)
        def _():
            most = xin.at[h, :, pl.ds(0, (NSEG - 1) * SEG)]
            pltpu.make_async_copy(most, most, recv_in.at[h]).wait()

        @pl.when(chip == 0)
        def _():
            pltpu.make_async_copy(xin.at[h], xin.at[h], recv_in.at[h]).wait()

        dqacc[...] = jnp.zeros_like(dqacc)

        for j in range(nblk):
            kr = pl.ds(j * BLK, BLK)

            def tile(i, masked):
                qr = pl.ds(pl.multiple_of(i * BLK, BLK), BLK)
                qb, dob = xin[h, 0, qr, :], xin[h, 3, qr, :]
                kb, vb = xin[h, 1, kr, :], xin[h, 2, kr, :]
                l2 = jnp.concatenate([ldin[i * per + s, pl.ds(h, 1), :] for s in range(per)], axis=1)
                dl = jnp.concatenate([ldin[i * per + s, pl.ds(hl + h, 1), :] for s in range(per)], axis=1)
                p = jnp.exp2(_nt(kb, qb) * (scale * LOG2E) - l2)
                if masked:
                    key = lax.broadcasted_iota(jnp.int32, (BLK, BLK), 0)
                    query = lax.broadcasted_iota(jnp.int32, (BLK, BLK), 1)
                    seen = key <= query
                    if j == nblk - 1:
                        seen = jnp.logical_and(seen, key < keys)
                    p = jnp.where(seen, p, 0.0)
                ds = (p * (_nt(vb, dob) - dl)).astype(BF16)
                dvb = _nn(p.astype(BF16), dob)
                dkb = _nn(ds, qb)
                dqacc[qr, :] += _tn(ds, kb)
                return dkb, dvb

            dkb, dvb = tile(j, True)
            dkacc[...] = dkb
            dvacc[...] = dvb

            @pl.loop(j + 1, nblk)
            def _(i):
                dkb, dvb = tile(i, False)
                dkacc[...] += dkb
                dvacc[...] += dvb

            obuf[h, 1, kr, :] = (dkacc[...] * scale).astype(BF16)
            obuf[h, 2, kr, :] = dvacc[...].astype(BF16)

        @pl.when(jnp.logical_and(outer, h == hl - 1))
        def _():
            pltpu.make_async_copy(pdq, pdq, pdq_sem).wait()
            dqacc[last, :] += pdq[...]

        obuf[h, 0] = (dqacc[...] * scale).astype(BF16)

        @pl.when(jnp.logical_and(outer, h < hl - 1))
        def _():
            fdq[h] = dqacc[last, :]
            for b in (0, 1):
                pltpu.make_async_remote_copy(fdq.at[h, pl.ds((1 - b) * SEG, SEG)], rdq.at[chip - 1, core, h], send_fdq, rdq_sem,
                                             device_id={'cp': b}, device_id_type=MESH).start()

        @pl.when(jnp.logical_and(chip == 0, h == 0))
        def _():
            forward()

        mine = me * hl + h
        for t, x in ((1, rin.at[0]), (2, rin.at[1]), (0, dqh)):
            for p in remote:
                for half, seg in ((0, p), (1, NSEG - 1 - p)):
                    src = obuf.at[h, t, pl.ds(pl.multiple_of(seg * SEG, SEG), SEG)]
                    go = me >= 0
                    if half == 1:
                        go = jnp.logical_not(jnp.logical_and(outer, p < 2))

                    @pl.when(go)
                    def _():
                        pltpu.make_async_remote_copy(src, x.at[mine, halves[half]], send_out, recv_out.at[t],
                                                     device_id={'cp': p}, device_id_type=MESH).start()

                    if half == 1 and t == 0:
                        @pl.when(jnp.logical_and(jnp.logical_not(go), h == hl - 1))
                        def _():
                            pltpu.make_async_remote_copy(src, x.at[mine, halves[half]], send_pdq, recv_out.at[t],
                                                         device_id={'cp': p}, device_id_type=MESH).start()
            for half in (0, 1):
                pltpu.make_async_copy(obuf.at[h, t, rows[half]], x.at[mine, halves[half]], recv_out.at[t]).start()
        return carry

    lax.fori_loop(0, hl, head, 0)

    for t, x in ((1, dk), (2, dv)):
        src = rin.at[t - 1]
        pltpu.make_async_copy(src, src, recv_out.at[t]).wait()
        for g in range(N // 2):
            heads = pl.ds(g * 2 * hl, 2 * hl)
            _swap(x.at[:, heads], src.at[heads], tok, inverse=True)

    @pl.when(chip == 0)
    def _():
        pltpu.make_async_copy(gdq, gdq, gdq_sem).wait()
        pltpu.make_async_copy(rdq, rdq, rdq_sem).wait()

        few = hl - 1

        @pl.loop(0, 6 * few)
        def _(i):
            c, b, h = i // (2 * few), (i // few) % 2, i % few
            total = gdq[c, b, h] + rdq[c, b, h]
            dqh[(2 * c + 2 + b) * hl + h, halves[1], :] = (total * scale).astype(BF16)

        some = dqh.at[pl.ds(0, 2 * N * hl // 2 - 3 * few)]
        pltpu.make_async_copy(some, some, recv_out.at[0]).wait()
        pltpu.make_async_copy(ldq.at[:, hl - 1], ldq.at[:, hl - 1], send_pdq).wait()
        for n, ref in enumerate((loc.at[:, :, :, halves[0]], locld.at[:, 0], lkv.at[:, :, :, halves[0]], ldq.at[:, first, halves[0]])):
            pltpu.make_async_copy(ref, ref, send_loc.at[n]).wait()
        pltpu.make_async_copy(rel, rel, fwd_sem).wait()
        sent = xin.at[:, :, pl.ds(0, 11 * SEG)]
        pltpu.make_async_copy(sent, sent, send_in).wait()
        sent = obuf.at[:, :, pl.ds(0, 14 * SEG)]
        pltpu.make_async_copy(sent, sent, send_out).wait()

    @pl.when(outer)
    def _():
        pltpu.make_async_copy(dqh, dqh, recv_out.at[0]).wait()
        pltpu.make_async_copy(fdq, fdq, send_fdq).wait()
        sent = obuf.at[hl - 1, 0, last]
        pltpu.make_async_copy(sent, sent, send_pdq).wait()
        sent = xin.at[:, :, pl.ds(0, 14 * SEG)]
        pltpu.make_async_copy(sent, sent, send_in).wait()
        sent = obuf.at[:, :, pl.ds(0, 12 * SEG)]
        pltpu.make_async_copy(sent, sent, send_out).wait()

    pltpu.make_async_copy(ldin.at[pl.ds(0, 2 * (N - 1))], ldin.at[pl.ds(0, 2 * (N - 1))], send_ld).wait()


def _close(dqh, dkt, dvt, dq, dk, dv, dqt, sem):
    heads, tok = dqh.shape[:2]
    parts = [pl.ds(i * CHUNK, CHUNK) for i in range(tok // CHUNK)]
    copies = [pltpu.make_async_copy(x.at[r], y.at[r], sem.at[n, i])
              for n, (x, y) in enumerate(((dkt, dk), (dvt, dv))) for i, r in enumerate(parts)]
    for copy in copies:
        copy.start()
    for i, r in enumerate(parts):
        for g in range(heads // 8):
            part = slice(g * 8, g * 8 + 8)
            dqt[i, :, part, :] = jnp.swapaxes(dqh[part, r, :], 0, 1)
        copies.append(pltpu.make_async_copy(dqt.at[i], dq.at[r], sem.at[2, i]))
        copies[-1].start()
    for copy in copies:
        copy.wait()


def solution(mesh):
    spec = P('data', 'cp', None, None)
    lspec = P('data', None, 'cp')

    def local(q, k, v, o, lse, do):
        b, tok, heads, dim = q.shape
        hl = heads // N
        any_ = pl.BlockSpec(memory_space=pltpu.HBM)
        vmem = pl.BlockSpec(memory_space=pltpu.VMEM)
        seq = NSEG * SEG
        outs = pl.pallas_call(
            functools.partial(_kernel, hl, dim ** -0.5),
            out_shape=[jax.ShapeDtypeStruct((heads, tok, dim), BF16)] + [jax.ShapeDtypeStruct((tok, heads, dim), BF16)] * 2,
            in_specs=[any_] * 6,
            out_specs=[vmem] * 3,
            scratch_shapes=[
                pltpu.VMEM((RING, tok, 2 * hl, dim), BF16),
                pltpu.VMEM((heads, tok), F32),
                pltpu.VMEM((4, N // 2, 2 * hl, tok, dim), BF16),
                pltpu.VMEM((2 * hl, tok, dim), BF16),
                pltpu.VMEM((N // 2, 2, 2, 2 * hl, SEG), F32),
                pltpu.VMEM((hl, 4, seq, dim), BF16),
                pltpu.VMEM((NSEG, 2 * hl, SEG), F32),
                pltpu.VMEM((hl, 3, seq, dim), BF16),
                pltpu.VMEM((2, heads, tok, dim), BF16),
                pltpu.VMEM((seq, dim), F32),
                pltpu.VMEM((BLK, dim), F32),
                pltpu.VMEM((BLK, dim), F32),
                pltpu.VMEM((5, tok, dim), BF16),
                pltpu.VMEM((3, 4, hl, 2 * SEG, dim), BF16),
                pltpu.VMEM((3, 2, 2 * hl, SEG), F32),
                pltpu.VMEM((2, 3, hl, 2 * SEG, dim), BF16),
                pltpu.VMEM((3, hl, 2 * SEG, dim), F32),
                pltpu.VMEM((3, 2, hl - 1, SEG, dim), F32),
                pltpu.VMEM((3, 2, hl - 1, SEG, dim), F32),
                pltpu.VMEM((hl - 1, 2 * SEG, dim), F32),
                pltpu.VMEM((2 * SEG, dim), F32),
                pltpu.SemaphoreType.DMA((RING,)),
                pltpu.SemaphoreType.DMA,
                pltpu.SemaphoreType.DMA,
                pltpu.SemaphoreType.DMA((hl,)),
                pltpu.SemaphoreType.DMA,
                pltpu.SemaphoreType.DMA,
                pltpu.SemaphoreType.DMA,
                pltpu.SemaphoreType.DMA((3,)),
                pltpu.SemaphoreType.DMA,
                pltpu.SemaphoreType.DMA,
                pltpu.SemaphoreType.DMA((4,)),
                pltpu.SemaphoreType.DMA((2,)),
                pltpu.SemaphoreType.DMA,
                pltpu.SemaphoreType.DMA,
                pltpu.SemaphoreType.DMA,
                pltpu.SemaphoreType.DMA,
                pltpu.SemaphoreType.DMA,
            ],
            compiler_params=pltpu.CompilerParams(collective_id=0, has_side_effects=True,
                                                 vmem_limit_bytes=46 * 2 ** 20),
            name='attention_backward',
        )(q[0], k[0], v[0], do[0], o[0], lse[0])
        grads = pl.pallas_call(
            _close,
            out_shape=[jax.ShapeDtypeStruct((tok, heads, dim), BF16)] * 3,
            in_specs=[vmem] * 3,
            out_specs=[any_] * 3,
            scratch_shapes=[pltpu.VMEM((tok // CHUNK, CHUNK, heads, dim), BF16),
                            pltpu.SemaphoreType.DMA((3, tok // CHUNK))],
            compiler_params=pltpu.CompilerParams(vmem_limit_bytes=16 * 2 ** 20),
            name='close',
        )(*outs)
        return tuple(x[None] for x in grads)

    return jax.shard_map(local, mesh=mesh, in_specs=(spec, spec, spec, spec, lspec, spec),
                         out_specs=(spec, spec, spec), check_vma=False)
```
